768 devices in a mesh: inter: 192 (over y, z, core), intra: 4 (over x).
Axes of the slice: x: 4, y: 8, z: 12, core: 2. Of those that a mesh axis runs over, the one named last changes fastest.
Arguments:
- partials: bfloat16 [768, 192, 5120], P(('inter', 'intra')), may hold values from -24 to 24
- scales: bfloat16 [768, 192, 20], P(('inter', 'intra')), may hold values from 64 to 1024
- overflow_pos: int32 [768, 1], P(('inter', 'intra')), may hold values from -983040 to 983039, as said below
- weights: float32 [192, 5120], P('inter', 'intra'), may hold values from -6 to 6
- exponent: int32 [], replicated, may hold values from 10 to 16
Outputs:
- grad_out: float32 [192, 5120], P('inter', 'intra')
- block_scale: float32 [192, 20], P('inter', 'intra')
- master_out: float32 [192, 5120], P('inter', 'intra')
- new_exponent: int32 [], replicated
- overflow_count: int32 [], replicated
The draws below stay inside these ranges and needn't reach their ends.
Inputs may be any that keep to these rules, and one draw needn't show every extreme that they name: `overflow_pos`: A negative entry means no overflow on that device; otherwise it is the flat position (row times 5120 plus column) of an overflowed value of that device's partial.
All inputs are finite; a program needn't handle non-finite values.
Results may differ from the reference program's by a relative error of at most 0.0005.
Values may be sent and summed in bfloat16 or wider, within the bound.
A program may use at most 64 MiB of HBM per device.

```python
import math
import jax
import jax.numpy as jnp
from jax import lax

D = 5120
BLOCK = 256
ROWS = 192
N_INTRA = 4
DEVICES = 768


def draw_overflow_pos(key, part):
    key_lead, key_more, key_pos, key_neg, key_pick = jax.random.split(jax.random.fold_in(key, 71), 5)
    group_total = DEVICES // N_INTRA
    negative = jax.random.randint(key_neg, (DEVICES, 1), -(ROWS * D), 0, dtype=jnp.int32)
    picked_device = jax.random.randint(key_pick, (), 0, DEVICES, dtype=jnp.int32)
    lead_member = jax.random.randint(key_lead, (group_total,), 0, N_INTRA, dtype=jnp.int32)
    member = jnp.arange(DEVICES, dtype=jnp.int32) % N_INTRA
    is_lead = member == jnp.repeat(lead_member, N_INTRA)
    extra_flag = jax.random.randint(key_more, (DEVICES,), 0, 2, dtype=jnp.int32) == 1
    flagged = jnp.logical_or(is_lead, extra_flag)
    positive = jax.random.randint(key_pos, (DEVICES, 1), 0, ROWS * D, dtype=jnp.int32)
    values = jnp.where(flagged[:, None], positive, negative)
    values = values.at[picked_device, 0].set(jnp.where(is_lead[picked_device], values[picked_device, 0], -(ROWS * D)))
    top_group = picked_device // N_INTRA
    top_device = top_group * N_INTRA + lead_member[top_group]
    return values.at[top_device, 0].set(ROWS * D - 1)


def spiked(array, key, source, target, blocks, factor):
    def block_of(axis_at):
        return (jnp.arange(array.shape[axis_at]) // (array.shape[axis_at] // blocks)).reshape((-1,) + (1,) * (array.ndim - 1 - axis_at))

    first = jax.random.permutation(key, blocks)[block_of(target)]
    far = (block_of(target) + blocks // 2) % blocks
    return jnp.where((block_of(source) == first) | (block_of(source) == far), factor * array, array)


def level_of(rng, extent, shards, low, top_value):
    gain, own = 1.0, jax.random.fold_in(rng, 6)
    for axis_at, parts in shards:
        heights = jnp.exp(jax.random.uniform(jax.random.fold_in(own, axis_at), (parts,), jnp.float32, low / len(shards), top_value / len(shards)))
        gain = gain * jnp.repeat(heights, extent[axis_at] // parts).reshape([-1 if axis == axis_at else 1 for axis in range(len(extent))])
    return gain


def gaussian(stream_key, shape, spread, reach, cuts=(), kind=jnp.bfloat16):
    factor_of = level_of(stream_key, shape, cuts, -0.22, 0.18) if cuts else 1.0
    values = jax.random.normal(stream_key, shape, jnp.float32) * spread * factor_of
    return jnp.minimum(jnp.maximum(values, -reach), reach).astype(kind)


def bell_draw_with(own_key, shape, deviation, reach, cuts, heavy, held_as=jnp.bfloat16):
    entries = deviation * jax.random.normal(own_key, shape, jnp.float32)
    if cuts:
        entries = entries * level_of(own_key, shape, cuts, -0.22, 0.18)
    return jnp.clip(spiked(entries, jax.random.fold_in(own_key, 3), *heavy), -reach, reach).astype(held_as)


def setup_inputs(seed: int = 0) -> dict:
    key_of = jax.random.split(jax.random.key(seed), 6)
    partials = bell_draw_with(key_of[0], (DEVICES, ROWS, D), 1.0, 24.0, ((0, 768),), (0, 1, 192, 6.0))
    scales = jnp.clip(jnp.exp(math.log(1024.0) - 2.7725887 * jax.random.uniform(key_of[1], (DEVICES, ROWS, D // BLOCK), jnp.float32) ** level_of(key_of[1], (DEVICES, ROWS, D // BLOCK), ((0, 768),), -0.2, 0.2)), 64.0, 1024.0).astype(jnp.bfloat16)
    overflow_pos = draw_overflow_pos(jax.random.fold_in(key_of[5], 71), 0)
    weights = gaussian(key_of[3], (ROWS, D), 1.0, 6.0, ((0, 192), (1, 4)), jnp.float32)
    exponent = jax.random.randint(key_of[4], (), 10, 17).astype(jnp.int32)
    return dict(partials=partials, scales=scales, overflow_pos=overflow_pos, weights=weights, exponent=exponent)


def reference(partials, scales, overflow_pos, weights, exponent):
    def add_term(grad_acc, inputs):
        levels, block_scales = inputs
        scaled = levels.astype(jnp.float32).reshape(ROWS, D // BLOCK, BLOCK) * block_scales.astype(jnp.float32)[:, :, None]
        return grad_acc + scaled.reshape(ROWS, D), None

    grad_sum, _ = lax.scan(add_term, jnp.zeros((ROWS, D), jnp.float32), (partials, scales))
    flag_count = jnp.sum((overflow_pos >= 0).astype(jnp.int32))
    grad_out = grad_sum * jnp.exp2(-exponent.astype(jnp.float32))
    block_scale = jnp.max(jnp.abs(grad_out.reshape(ROWS, D // BLOCK, BLOCK)), axis=2) / 127.0
    master_out = jnp.where(flag_count == 0, weights - 0.5 * grad_out, weights)
    new_exponent = exponent - (flag_count > 0).astype(jnp.int32)
    return grad_out, block_scale, master_out, new_exponent, flag_count
```

```python
import functools

import jax
import jax.numpy as jnp
from jax import lax
from jax.experimental import pallas as pl
from jax.experimental.pallas import tpu as pltpu
from jax.sharding import PartitionSpec as P

MESH = pl.DeviceIdType.MESH
NX, NY, NZ = 4, 8, 12
ZC = 2 * NZ
TI, TJ = ZC // 8, 5
HALF = TJ * 128
TOP = 32767.0


def wait(ref, sem):
    pltpu.make_async_copy(ref, ref, sem).wait()


def far_first(k, n):
    m = (k + 1) // 2
    return jnp.where(k % 2 == 1, n // 2 - m, n // 2 + m)


def encode(tiles, out):
    lane = lax.broadcasted_iota(jnp.int32, (8, 128), 1)
    tops = jnp.zeros((8, 128), jnp.float32)
    flat = []
    for row in tiles:
        peak = functools.reduce(jnp.maximum, [jnp.abs(t) for t in row])
        peak = jnp.maximum(jnp.max(peak, axis=1, keepdims=True), 1e-30)
        top = jnp.ceil(jnp.log2(jnp.broadcast_to(peak, (8, 128))) + 1e-3)
        tops = jnp.where(lane == len(flat) // TJ, top, tops)
        factor = jnp.exp2(-top) * TOP
        flat += [t * factor for t in row]
    flat.append(tops)
    for p in range(len(flat) // 2):
        pair = jnp.concatenate([flat[2 * p], flat[2 * p + 1]], axis=0)
        out[p] = jnp.round(pair).astype(jnp.int32).astype(jnp.int16)


def decode(ref):
    flat = []
    for p in range((TI * TJ + 1) // 2):
        pair = ref[p].astype(jnp.int32).astype(jnp.float32)
        flat += [pair[:8], pair[8:]]
    factors = jnp.exp2(flat[TI * TJ]) * (1.0 / TOP)
    return [
        [flat[i * TJ + j] * jnp.broadcast_to(factors[:, i : i + 1], (8, 128)) for j in range(TJ)]
        for i in range(TI)
    ]


def add(a, b):
    return [[p + q for p, q in zip(r, s)] for r, s in zip(a, b)]


def kernel(
    part, scales, pos, weights, exponent,
    grad, block_scale, master, new_exponent, count,
    lev, par, sc, sco, xs, xr, xo, ys, yr, zs, zr, fs, fx, fy,
    load_sem, sc_sem, core_send, core_recv, x_send, x_recv, y_send, y_recv, z_send, z_recv,
    fx_send, fx_recv, fy_send, fy_recv,
):
    inter, x = lax.axis_index("inter"), lax.axis_index("intra")
    c, zc = inter % 2, inter % ZC
    z, y = zc // 2, inter // ZC
    partner = inter + 1 - 2 * c

    for h, side in ((1, 1 - c), (0, c)):
        for xt in range(NX):
            columns = pl.ds(pl.multiple_of(xt * 2 * HALF + side * HALF, 128), HALF)
            pltpu.make_async_copy(part.at[:, :, :, columns], lev.at[h, :, xt], load_sem.at[h]).start()
    pltpu.make_async_copy(scales, sc.at[0], sc_sem.at[0]).start()

    barrier = pltpu.get_barrier_semaphore()

    def meet(to):
        pl.semaphore_signal(barrier, inc=1, device_id=to, device_id_type=MESH)

    for d in range(1, NX):
        meet((inter, (x + d) % NX))
    for d in range(1, NY):
        meet(((y + d) % NY * ZC + zc, x))
    for d in range(1, ZC):
        meet((y * ZC + (zc + d) % ZC, x))
    fs[0] = jnp.full((1, 128), (pos[0, 0] >= 0).astype(jnp.float32), jnp.float32)
    wait(sc.at[0], sc_sem.at[0])
    wait(lev.at[1], load_sem.at[1])
    pl.semaphore_wait(barrier, NX - 1 + NY - 1 + ZC - 1)

    def core_copy(k):
        yt = (y + far_first(k, NY)) % NY
        return pltpu.make_async_remote_copy(
            lev.at[1, yt], par.at[yt], core_send.at[k], core_recv.at[k], (partner, x), MESH
        )

    scale_copy = pltpu.make_async_remote_copy(
        sc.at[0], sc.at[1], sc_sem.at[1], sc_sem.at[2], (partner, x), MESH
    )
    scale_copy.start()

    @pl.loop(0, NY)
    def _(k):
        core_copy(k).start()

    def flag_x(d):
        return pltpu.make_async_remote_copy(
            fs.at[0], fx.at[d - 1], fx_send.at[d - 1], fx_recv.at[d - 1], (inter, (x + d) % NX), MESH
        )

    for d in range(1, NX):
        flag_x(d).start()
    wait(lev.at[0], load_sem.at[0])
    scale_copy.wait()

    def widen(h):
        @pl.loop(0, NY)
        def _(g):
            for i in range(TI):
                sco[h, g, i, :, 0:20] = sc[h, g, i].astype(jnp.float32)

    widen(0)
    widen(1)

    def x_copy(k, d):
        return pltpu.make_async_remote_copy(
            xs.at[k, d - 1], xr.at[k, d - 1], x_send, x_recv.at[k], (inter, (x + d) % NX), MESH
        )

    @pl.loop(0, NY)
    def _(k):
        yt = (y + far_first(k, NY)) % NY
        wait(par.at[yt], core_recv.at[k])
        for d in (2, 1, 3, 0):
            xt = (x + d) % NX
            shift = (128 - (xt * TJ + 2 * c)) % 128
            tiles = []
            for i in range(TI):
                total = None
                for h in range(2):
                    s = pltpu.roll(sco[h, yt, i], shift, 1)
                    b = [jnp.broadcast_to(s[:, n : n + 1], (8, 128)) for n in range(3)]
                    even = c == 0
                    b = [b[0], jnp.where(even, b[0], b[1]), b[1], jnp.where(even, b[1], b[2]), b[2]]
                    levels = lev[0, yt, xt, i] if h == 0 else par[yt, xt, i]
                    levels = levels.astype(jnp.float32)
                    term = [levels[:, j * 128 : (j + 1) * 128] * b[j] for j in range(TJ)]
                    total = term if total is None else [p + q for p, q in zip(total, term)]
                tiles.append(total)
            if d:
                encode(tiles, xs.at[k, d - 1])
                x_copy(k, d).start()
            else:
                for i in range(TI):
                    for j in range(TJ):
                        xo[k, i * TJ + j] = tiles[i][j]

    flags = fs[0]
    for d in range(1, NX):
        wait(fx.at[d - 1], fx_recv.at[d - 1])
        flags = flags + fx[d - 1]
    fs[1] = flags

    def flag_y(d):
        return pltpu.make_async_remote_copy(
            fs.at[1], fy.at[d - 1], fy_send.at[d - 1], fy_recv.at[d - 1], ((y + d) % NY * ZC + zc, x), MESH
        )

    for d in range(1, NY):
        flag_y(d).start()

    def y_copy(k):
        return pltpu.make_async_remote_copy(
            ys.at[k], yr.at[k], y_send.at[k], y_recv.at[k], ((y + far_first(k, NY)) % NY * ZC + zc, x), MESH
        )

    def x_sum(k):
        wait(xr.at[k], x_recv.at[k])
        tiles = [[xo[k, i * TJ + j] for j in range(TJ)] for i in range(TI)]
        for d in range(1, NX):
            tiles = add(tiles, decode(xr.at[k, d - 1]))
        return tiles

    @pl.loop(0, NY - 1)
    def _(k):
        encode(x_sum(k), ys.at[k])
        y_copy(k).start()

    tiles = x_sum(NY - 1)
    for d in range(1, NY):
        wait(fy.at[d - 1], fy_recv.at[d - 1])
        flags = flags + fy[d - 1]
    for k in range(NY - 1):
        wait(yr.at[k], y_recv.at[k])
        tiles = add(tiles, decode(yr.at[k]))
    for i in range(TI):
        for j in range(TJ):
            zs[pl.ds(i * 64 + j, 8, stride=8), :] = tiles[i][j]
        zs[pl.ds(i * 64 + TJ, 8, stride=8), :] = jnp.broadcast_to(flags, (8, 128))

    def rows(n):
        return pl.ds(pl.multiple_of(n * 8, 8), TJ + 1)

    def z_copy(k):
        to = (zc + far_first(k, ZC)) % ZC
        return pltpu.make_async_remote_copy(
            zs.at[rows(to)], zr.at[rows(zc)], z_send.at[k], z_recv.at[k], (y * ZC + to, x), MESH
        )

    @pl.loop(0, ZC - 1)
    def _(k):
        z_copy(k).start()

    own = pl.ds(pl.multiple_of(zc * 8, 8), 8)
    mine = zs[own, :]

    for d in range(1, NX):
        wait(fs.at[0], fx_send.at[d - 1])
    for d in range(1, NY):
        wait(fs.at[1], fy_send.at[d - 1])
    wait(xs, x_send)

    @pl.loop(0, NY)
    def _(k):
        wait(lev.at[1, k], core_send.at[k])

    @pl.loop(0, NY - 1)
    def _(k):
        wait(ys.at[k], y_send.at[k])

    @pl.loop(0, ZC - 1)
    def _(k):
        wait(zr.at[rows(k)], z_recv.at[k])

    zr[own, :] = mine
    halves = [
        functools.reduce(jnp.add, [zr[(2 * n + h) * 8 : (2 * n + h) * 8 + 8, :] for n in range(NZ)])
        for h in range(2)
    ]
    total = halves[0][TJ, 0] + halves[1][TJ, 0]
    flagged = total.astype(jnp.int32)
    factor = jnp.exp2(jnp.full((8, 128), -exponent[0].astype(jnp.float32), jnp.float32))
    peaks = []
    for h in range(2):
        g = halves[h] * factor
        peak = jnp.max(jnp.abs(g), axis=1, keepdims=True)
        for j in range(TJ):
            at = slice((h * TJ + j) * 128, (h * TJ + j + 1) * 128)
            w = weights[:, at]
            grad[:, at] = g[j : j + 1]
            master[:, at] = jnp.where(flagged == 0, w - 0.5 * g[j : j + 1], w)
            peaks.append(peak[j : j + 1])
    lane = lax.broadcasted_iota(jnp.int32, (1, 128), 1)
    scale = jnp.zeros((1, 128), jnp.float32)
    for b in range(TJ):
        top = jnp.maximum(peaks[2 * b], peaks[2 * b + 1]) / 127.0
        scale = jnp.where(lane == b, jnp.broadcast_to(top, (1, 128)), scale)
    block_scale[...] = scale[:, :TJ]
    new_exponent[0] = exponent[0] - (flagged > 0).astype(jnp.int32)
    count[0] = flagged

    @pl.loop(0, ZC - 1)
    def _(k):
        wait(zr.at[rows(k)], z_send.at[k])


def on_device(partials, scales, overflow_pos, weights, exponent):
    vmem, smem, anywhere = (
        pl.BlockSpec(memory_space=m) for m in (pltpu.VMEM, pltpu.SMEM, pl.ANY)
    )
    f32, i16, dma = jnp.float32, jnp.int16, pltpu.SemaphoreType.DMA
    code = (8, 16, 128)
    grad, block_scale, master, new_exponent, count = pl.pallas_call(
        kernel,
        out_shape=(
            jax.ShapeDtypeStruct((1, 2 * HALF), f32),
            jax.ShapeDtypeStruct((1, TJ), f32),
            jax.ShapeDtypeStruct((1, 2 * HALF), f32),
            jax.ShapeDtypeStruct((1,), jnp.int32),
            jax.ShapeDtypeStruct((1,), jnp.int32),
        ),
        in_specs=[anywhere, anywhere, smem, vmem, smem],
        out_specs=[vmem, vmem, vmem, smem, smem],
        scratch_shapes=[
            pltpu.VMEM((2, NY, NX, TI, 8, HALF), jnp.bfloat16),
            pltpu.VMEM((NY, NX, TI, 8, HALF), jnp.bfloat16),
            pltpu.VMEM((2, NY, TI, 8, 20), jnp.bfloat16),
            pltpu.VMEM((2, NY, TI, 8, 128), f32),
            pltpu.VMEM((NY, NX - 1, *code), i16),
            pltpu.VMEM((NY, NX - 1, *code), i16),
            pltpu.VMEM((NY, TI * TJ, 8, 128), f32),
            pltpu.VMEM((NY - 1, *code), i16),
            pltpu.VMEM((NY - 1, *code), i16),
            pltpu.VMEM((ZC * 8, 128), f32),
            pltpu.VMEM((ZC * 8, 128), f32),
            pltpu.VMEM((2, 1, 128), f32),
            pltpu.VMEM((NX - 1, 1, 128), f32),
            pltpu.VMEM((NY - 1, 1, 128), f32),
            dma((2,)), dma((3,)), dma((NY,)), dma((NY,)), dma, dma((NY,)),
            dma((NY - 1,)), dma((NY - 1,)), dma((ZC - 1,)), dma((ZC - 1,)),
            dma((NX - 1,)), dma((NX - 1,)), dma((NY - 1,)), dma((NY - 1,)),
        ],
        compiler_params=pltpu.CompilerParams(collective_id=0, has_side_effects=True),
    )(
        partials.reshape(NY, TI, 8, partials.shape[2]),
        scales.reshape(NY, TI, 8, scales.shape[2]),
        overflow_pos,
        weights,
        exponent.reshape(1),
    )
    return grad, block_scale, master, new_exponent.reshape(()), count.reshape(())


def solution(mesh):
    return jax.shard_map(
        on_device,
        mesh=mesh,
        in_specs=(
            P(("inter", "intra"), None, None),
            P(("inter", "intra"), None, None),
            P(("inter", "intra"), None),
            P("inter", "intra"),
            P(),
        ),
        out_specs=(P("inter", "intra"), P("inter", "intra"), P("inter", "intra"), P(), P()),
        check_vma=False,
    )
```

```python
import functools

import jax
import jax.numpy as jnp
from jax import lax
from jax.experimental import pallas as pl
from jax.experimental.pallas import tpu as pltpu
from jax.sharding import PartitionSpec as P

MESH = pl.DeviceIdType.MESH
NX, NY, NZ = 4, 8, 12
ZC = 2 * NZ
TI, TJ = ZC // 8, 5
HALF = TJ * 128
TOP = 32767.0


def wait(ref, sem):
    pltpu.make_async_copy(ref, ref, sem).wait()


def far_first(k, n):
    m = (k + 1) // 2
    return jnp.where(k % 2 == 1, n // 2 - m, n // 2 + m)


def encode(tiles, out):
    lane = lax.broadcasted_iota(jnp.int32, (8, 128), 1)
    tops = jnp.zeros((8, 128), jnp.float32)
    flat = []
    for row in tiles:
        peak = functools.reduce(jnp.maximum, [jnp.abs(t) for t in row])
        peak = jnp.maximum(jnp.max(peak, axis=1, keepdims=True), 1e-30)
        top = jnp.ceil(jnp.log2(jnp.broadcast_to(peak, (8, 128))) + 1e-3)
        tops = jnp.where(lane == len(flat) // TJ, top, tops)
        factor = jnp.exp2(-top) * TOP
        flat += [t * factor for t in row]
    flat.append(tops)
    for p in range(len(flat) // 2):
        pair = jnp.concatenate([flat[2 * p], flat[2 * p + 1]], axis=0)
        out[p] = jnp.round(pair).astype(jnp.int32).astype(jnp.int16)


def decode(ref):
    flat = []
    for p in range((TI * TJ + 1) // 2):
        pair = ref[p].astype(jnp.int32).astype(jnp.float32)
        flat += [pair[:8], pair[8:]]
    factors = jnp.exp2(flat[TI * TJ]) * (1.0 / TOP)
    return [
        [flat[i * TJ + j] * jnp.broadcast_to(factors[:, i : i + 1], (8, 128)) for j in range(TJ)]
        for i in range(TI)
    ]


def add(a, b):
    return [[p + q for p, q in zip(r, s)] for r, s in zip(a, b)]


def kernel(
    part, scales, pos, exponent,
    out,
    lev, par, sc, st, sco, flag, power, xs, xr, xo, ys, yr, zs, zr, fs, fx, fy,
    load_sem, sc_sem, flag_sem, power_sem, near, core_send, core_recv, x_send, x_recv, y_send, y_recv, z_send, z_recv,
    fx_send, fx_recv, fy_send, fy_recv,
):
    inter, x = lax.axis_index("inter"), lax.axis_index("intra")
    c, zc = inter % 2, inter % ZC
    z, y = zc // 2, inter // ZC
    partner = inter + 1 - 2 * c

    for h, side in ((1, 1 - c), (0, c)):
        for xt in range(NX):
            columns = pl.ds(pl.multiple_of(xt * 2 * HALF + side * HALF, 128), HALF)
            pltpu.make_async_copy(part.at[:, :, :, columns], lev.at[h, :, xt], load_sem.at[h]).start()
    pltpu.make_async_copy(scales, sc.at[0], sc_sem.at[0]).start()

    pltpu.make_async_copy(pos, flag, flag_sem).start()
    pltpu.make_async_copy(exponent, power, power_sem).start()

    barrier = pltpu.get_barrier_semaphore()

    def along_y(d):
        return ((y + d) % NY * ZC + zc, x)

    def along_z(d):
        return (y * ZC + (zc + 2 * d) % ZC, x)

    def tell(sem, to):
        pl.semaphore_signal(sem, inc=1, device_id=to, device_id_type=MESH)

    def tell_both(sem, along, n, d):
        tell(near.at[sem], along(d))
        tell(near.at[sem], along(n - d))

    tell(barrier, (partner, x))
    for d in range(1, NX):
        tell(barrier, (inter, (x + d) % NX))
    for d in (1, NY - 1):
        tell(barrier, along_y(d))
    for d in (1, NZ - 1):
        tell(barrier, along_z(d))
    with jax.named_scope("load"):
        wait(sc.at[0], sc_sem.at[0])
        wait(lev.at[1], load_sem.at[1])
    with jax.named_scope("barrier"):
        pl.semaphore_wait(barrier, 1 + NX - 1 + 2 + 2)
    tell_both(0, along_y, NY, 1)
    tell_both(1, along_z, NZ, 1)

    def core_copy(k):
        yt = (y + far_first(k, NY)) % NY
        return pltpu.make_async_remote_copy(
            lev.at[1, yt], par.at[yt], core_send.at[k], core_recv.at[k], (partner, x), MESH
        )

    scale_copy = pltpu.make_async_remote_copy(
        sc.at[0], sc.at[1], sc_sem.at[1], sc_sem.at[2], (partner, x), MESH
    )
    scale_copy.start()

    @pl.loop(0, NY)
    def _(k):
        core_copy(k).start()

    def flag_x(d):
        return pltpu.make_async_remote_copy(
            fs.at[0], fx.at[d - 1], fx_send.at[d - 1], fx_recv.at[d - 1], (inter, (x + d) % NX), MESH
        )

    wait(flag, flag_sem)
    wait(power, power_sem)
    fs[0] = jnp.full((1, 128), (flag[0, 0] >= 0).astype(jnp.float32), jnp.float32)
    for d in range(1, NX):
        flag_x(d).start()
    with jax.named_scope("wait_scale"):
        wait(lev.at[0], load_sem.at[0])
        scale_copy.wait()

    with jax.named_scope("scales"):
        for h in range(2):
            st[h, :20, : NY * ZC] = sc[h].astype(jnp.float32)
            for r in range(0, NY * ZC, 128):
                n = min(128, NY * ZC - r) // 8
                sco[h, r // 8 : r // 8 + n, :, :32] = st[h, :, r : r + 128].T.reshape(16, 8, 32)[:n]

    def x_copy(k, d):
        return pltpu.make_async_remote_copy(
            xs.at[k, d - 1], xr.at[k, d - 1], x_send, x_recv.at[k], (inter, (x + d) % NX), MESH
        )

    @pl.loop(0, NY)
    def _(k):
        yt = (y + far_first(k, NY)) % NY
        with jax.named_scope("wait_core"):
            wait(par.at[yt], core_recv.at[k])
        for d in (2, 1, 3, 0):
            xt = (x + d) % NX
            shift = (128 - (xt * TJ + 2 * c)) % 128
            tiles = []
            for i in range(TI):
                total = None
                for h in range(2):
                    s = pltpu.roll(sco[h, yt * TI + i], shift, 1)
                    b = [jnp.broadcast_to(s[:, n : n + 1], (8, 128)) for n in range(3)]
                    even = c == 0
                    b = [b[0], jnp.where(even, b[0], b[1]), b[1], jnp.where(even, b[1], b[2]), b[2]]
                    levels = lev[0, yt, xt, i] if h == 0 else par[yt, xt, i]
                    levels = levels.astype(jnp.float32)
                    term = [levels[:, j * 128 : (j + 1) * 128] * b[j] for j in range(TJ)]
                    total = term if total is None else [p + q for p, q in zip(total, term)]
                tiles.append(total)
            if d:
                encode(tiles, xs.at[k, d - 1])
                x_copy(k, d).start()
            else:
                for i in range(TI):
                    for j in range(TJ):
                        xo[k, i * TJ + j] = tiles[i][j]

    pl.semaphore_wait(near.at[0], 2)
    pl.semaphore_wait(near.at[1], 2)
    tell_both(2, along_y, NY, 2)
    tell_both(3, along_z, NZ, 2)

    flags = fs[0]
    for d in range(1, NX):
        wait(fx.at[d - 1], fx_recv.at[d - 1])
        flags = flags + fx[d - 1]
    fs[1] = flags
    with jax.named_scope("near"):
        pl.semaphore_wait(near.at[2], 2)
        pl.semaphore_wait(near.at[3], 2)
    tell_both(4, along_z, NZ, 4)

    def flag_y(d):
        return pltpu.make_async_remote_copy(
            fs.at[1], fy.at[d - 1], fy_send.at[d - 1], fy_recv.at[d - 1], along_y(d), MESH
        )

    for d in range(1, NY):
        flag_y(d).start()

    def y_copy(k):
        return pltpu.make_async_remote_copy(
            ys.at[k], yr.at[k], y_send.at[k], y_recv.at[k], along_y(far_first(k, NY)), MESH
        )

    def x_sum(k):
        with jax.named_scope("wait_x"):
            wait(xr.at[k], x_recv.at[k])
        tiles = [[xo[k, i * TJ + j] for j in range(TJ)] for i in range(TI)]
        for d in range(1, NX):
            tiles = add(tiles, decode(xr.at[k, d - 1]))
        return tiles

    @pl.loop(0, NY - 1)
    def _(k):
        encode(x_sum(k), ys.at[k])
        y_copy(k).start()

    tiles = x_sum(NY - 1)
    for d in range(1, NY):
        wait(fy.at[d - 1], fy_recv.at[d - 1])
        flags = flags + fy[d - 1]
    for k in range(NY - 1):
        with jax.named_scope("wait_y"):
            wait(yr.at[k], y_recv.at[k])
        tiles = add(tiles, decode(yr.at[k]))
    for i in range(TI):
        for j in range(TJ):
            zs[pl.ds(i * 64 + j, 8, stride=8), :] = tiles[i][j]
        zs[pl.ds(i * 64 + TJ, 8, stride=8), :] = jnp.broadcast_to(flags, (8, 128))

    def rows(n):
        return pl.ds(pl.multiple_of(n * 8, 8), TJ + 1)

    def z_copy(k):
        to = (zc + far_first(k, ZC)) % ZC
        return pltpu.make_async_remote_copy(
            zs.at[rows(to)], zr.at[rows(zc)], z_send.at[k], z_recv.at[k], (y * ZC + to, x), MESH
        )

    pl.semaphore_wait(near.at[4], 2)

    @pl.loop(0, ZC - 1)
    def _(k):
        z_copy(k).start()

    own = pl.ds(pl.multiple_of(zc * 8, 8), 8)
    mine = zs[own, :]

    for d in range(1, NX):
        wait(fs.at[0], fx_send.at[d - 1])
    for d in range(1, NY):
        wait(fs.at[1], fy_send.at[d - 1])
    wait(xs, x_send)

    @pl.loop(0, NY)
    def _(k):
        wait(lev.at[1, k], core_send.at[k])

    @pl.loop(0, NY - 1)
    def _(k):
        wait(ys.at[k], y_send.at[k])

    with jax.named_scope("wait_z"):

        @pl.loop(0, ZC - 1)
        def _(k):
            wait(zr.at[rows(k)], z_recv.at[k])

    zr[own, :] = mine
    for h in range(2):
        out[h * 8 : h * 8 + 8, :] = functools.reduce(
            jnp.add, [zr[(2 * n + h) * 8 : (2 * n + h) * 8 + 8, :] for n in range(NZ)]
        )
    out[7:8, :] = jnp.full((1, 128), power[0].astype(jnp.float32), jnp.float32)

    @pl.loop(0, ZC - 1)
    def _(k):
        wait(zr.at[rows(k)], z_send.at[k])


def finish(sums, weights, grad, block_scale, master, new_exponent, count):
    total = sums[TJ, 0] + sums[8 + TJ, 0]
    flagged = total.astype(jnp.int32)
    factor = jnp.exp2(-jnp.broadcast_to(sums[7:8, :], (8, 128)))
    peaks = []
    for h in range(2):
        g = sums[h * 8 : h * 8 + 8, :] * factor
        peak = jnp.max(jnp.abs(g), axis=1, keepdims=True)
        for j in range(TJ):
            at = slice((h * TJ + j) * 128, (h * TJ + j + 1) * 128)
            w = weights[:, at]
            grad[:, at] = g[j : j + 1]
            master[:, at] = jnp.where(flagged == 0, w - 0.5 * g[j : j + 1], w)
            peaks.append(peak[j : j + 1])
    lane = lax.broadcasted_iota(jnp.int32, (1, 128), 1)
    scale = jnp.zeros((1, 128), jnp.float32)
    for b in range(TJ):
        top = jnp.maximum(peaks[2 * b], peaks[2 * b + 1]) / 127.0
        scale = jnp.where(lane == b, jnp.broadcast_to(top, (1, 128)), scale)
    block_scale[...] = scale[:, :TJ]
    new_exponent[0] = sums[7, 0].astype(jnp.int32) - (flagged > 0).astype(jnp.int32)
    count[0] = flagged


def on_device(partials, scales, overflow_pos, weights, exponent):
    vmem, smem, hbm = (
        pl.BlockSpec(memory_space=m) for m in (pltpu.VMEM, pltpu.SMEM, pltpu.HBM)
    )
    f32, i16, dma = jnp.float32, jnp.int16, pltpu.SemaphoreType.DMA
    code = (8, 16, 128)
    sums = pl.pallas_call(
        kernel,
        out_shape=jax.ShapeDtypeStruct((16, 128), f32),
        in_specs=[hbm] * 4,
        out_specs=vmem,
        scratch_shapes=[
            pltpu.VMEM((2, NY, NX, TI, 8, HALF), jnp.bfloat16),
            pltpu.VMEM((NY, NX, TI, 8, HALF), jnp.bfloat16),
            pltpu.VMEM((2, 20, NY * ZC), jnp.bfloat16),
            pltpu.VMEM((2, 32, 256), f32),
            pltpu.VMEM((2, NY * TI, 8, 128), f32),
            pltpu.SMEM((1, 1), jnp.int32),
            pltpu.SMEM((1,), jnp.int32),
            pltpu.VMEM((NY, NX - 1, *code), i16),
            pltpu.VMEM((NY, NX - 1, *code), i16),
            pltpu.VMEM((NY, TI * TJ, 8, 128), f32),
            pltpu.VMEM((NY - 1, *code), i16),
            pltpu.VMEM((NY - 1, *code), i16),
            pltpu.VMEM((ZC * 8, 128), f32),
            pltpu.VMEM((ZC * 8, 128), f32),
            pltpu.VMEM((2, 1, 128), f32),
            pltpu.VMEM((NX - 1, 1, 128), f32),
            pltpu.VMEM((NY - 1, 1, 128), f32),
            dma((2,)), dma((3,)), dma, dma, pltpu.SemaphoreType.REGULAR((5,)), dma((NY,)), dma((NY,)), dma, dma((NY,)),
            dma((NY - 1,)), dma((NY - 1,)), dma((ZC - 1,)), dma((ZC - 1,)),
            dma((NX - 1,)), dma((NX - 1,)), dma((NY - 1,)), dma((NY - 1,)),
        ],
        compiler_params=pltpu.CompilerParams(collective_id=0, has_side_effects=True),
        name="exchange",
    )(
        partials.reshape(NY, TI, 8, partials.shape[2]),
        scales.reshape(scales.shape[1:]).T,
        overflow_pos,
        exponent.reshape(1),
    )
    grad, block_scale, master, new_exponent, count = pl.pallas_call(
        finish,
        out_shape=(
            jax.ShapeDtypeStruct((1, 2 * HALF), f32),
            jax.ShapeDtypeStruct((1, TJ), f32),
            jax.ShapeDtypeStruct((1, 2 * HALF), f32),
            jax.ShapeDtypeStruct((1,), jnp.int32),
            jax.ShapeDtypeStruct((1,), jnp.int32),
        ),
        in_specs=[vmem, vmem],
        out_specs=[vmem, vmem, vmem, smem, smem],
        name="finish",
    )(sums, weights)
    return grad, block_scale, master, new_exponent.reshape(()), count.reshape(())


def solution(mesh):
    return jax.shard_map(
        on_device,
        mesh=mesh,
        in_specs=(
            P(("inter", "intra"), None, None),
            P(("inter", "intra"), None, None),
            P(("inter", "intra"), None),
            P("inter", "intra"),
            P(),
        ),
        out_specs=(P("inter", "intra"), P("inter", "intra"), P("inter", "intra"), P(), P()),
        check_vma=False,
    )
```

```python
import functools

import jax
import jax.numpy as jnp
from jax import lax
from jax.experimental import pallas as pl
from jax.experimental.pallas import tpu as pltpu
from jax.sharding import PartitionSpec as P

MESH = pl.DeviceIdType.MESH
NX, NY, NZ = 4, 8, 12
ZC = 2 * NZ
TI, TJ = ZC // 8, 5
HALF = TJ * 128
NB = 3
TOP = 32767.0
NS = NY - 3
FLAG_STEP = 3


def wait(ref, sem):
    pltpu.make_async_copy(ref, ref, sem).wait()


def far_first(k, n):
    m = (k + 1) // 2
    return jnp.where(k % 2 == 1, n // 2 - m, n // 2 + m)


def top_of(row):
    peak = functools.reduce(jnp.maximum, [jnp.abs(t) for t in row])
    peak = jnp.maximum(jnp.max(peak, axis=1, keepdims=True), 1e-30)
    return jnp.ceil(jnp.log2(jnp.broadcast_to(peak, (8, 128))) + 1e-3)


def code(values):
    return jnp.round(values).astype(jnp.int32).astype(jnp.int16)


def encode(tiles, tops, out):
    lane = lax.broadcasted_iota(jnp.int32, (8, 128), 1)
    flat, marks = [], jnp.zeros((8, 128), jnp.float32)
    for i in range(TI):
        factor = jnp.exp2(-tops[i]) * TOP
        flat += [t * factor for t in tiles[i]]
        marks = jnp.where(lane == i, tops[i], marks)
    flat.append(marks)
    for p in range(len(flat) // 2):
        out[p] = code(jnp.concatenate([flat[2 * p], flat[2 * p + 1]], axis=0))


def decode(ref):
    flat = []
    for p in range((TI * TJ + 1) // 2):
        pair = ref[p].astype(jnp.int32).astype(jnp.float32)
        flat += [pair[:8], pair[8:]]
    factors = jnp.exp2(flat[TI * TJ]) * (1.0 / TOP)
    return [
        [flat[i * TJ + j] * jnp.broadcast_to(factors[:, i : i + 1], (8, 128)) for j in range(TJ)]
        for i in range(TI)
    ]


def add(a, b):
    return [[p + q for p, q in zip(r, s)] for r, s in zip(a, b)]


def kernel(
    part, scales, pos, exponent, weights,
    out,
    lev, par, sc, st, turned, bx, flag, power, held, terms, cs, ms, xr, mr, ys, yr, zs, zq, zr, fs, fx, fy, fz,
    load_sem, sc_sem, flag_sem, power_sem, held_sem, near, core_send, core_recv, x_send, x_recv, m_send, m_recv, y_send, y_recv, z_send, z_recv,
    fx_send, fx_recv, fy_send, fy_recv, fz_send, fz_recv,
):
    inter, x = lax.axis_index("inter"), lax.axis_index("intra")
    c, zc = inter % 2, inter % ZC
    z, y = zc // 2, inter // ZC
    partner = inter + 1 - 2 * c

    for h, side in ((1, 1 - c), (0, c)):
        for xt in range(NX):
            columns = pl.ds(pl.multiple_of(xt * 2 * HALF + side * HALF, 128), HALF)
            pltpu.make_async_copy(part.at[:, :, :, columns], lev.at[h, :, xt], load_sem.at[h]).start()
    pltpu.make_async_copy(scales, sc.at[0], sc_sem.at[0]).start()

    pltpu.make_async_copy(pos, flag, flag_sem).start()
    pltpu.make_async_copy(exponent, power, power_sem).start()
    pltpu.make_async_copy(weights, held, held_sem).start()

    barrier = pltpu.get_barrier_semaphore()

    def along_y(d):
        return ((y + d) % NY * ZC + zc, x)

    def along_z(d):
        return (y * ZC + (zc + 2 * d) % ZC, x)

    def tell(sem, to):
        pl.semaphore_signal(sem, inc=1, device_id=to, device_id_type=MESH)

    def tell_both(sem, along, n, d):
        tell(near.at[sem], along(d))
        tell(near.at[sem], along(n - d))

    tell(barrier, (partner, x))
    for d in range(1, NX):
        tell(barrier, (inter, (x + d) % NX))
    for d in (1, NY - 1):
        tell(barrier, along_y(d))
    for d in (1, NZ - 1):
        tell(barrier, along_z(d))
    with jax.named_scope("load"):
        wait(sc.at[0], sc_sem.at[0])
        wait(lev.at[1], load_sem.at[1])
    with jax.named_scope("barrier"):
        pl.semaphore_wait(barrier, 1 + NX - 1 + 2 + 2)
    tell_both(0, along_y, NY, 1)
    tell_both(1, along_z, NZ, 1)

    def offset(q):
        late = far_first(q - 2, NY)
        return jnp.where(q == 0, NY // 2, jnp.where(q == 1, 1, jnp.where(q == 2, NY - 1, jnp.where(q == NY - 1, 0, late))))

    def core_copy(k):
        yt = (y + offset(k)) % NY
        return pltpu.make_async_remote_copy(
            lev.at[1, yt], par.at[yt], core_send, core_recv.at[k], (partner, x), MESH
        )

    scale_copy = pltpu.make_async_remote_copy(
        sc.at[0], sc.at[1], sc_sem.at[1], sc_sem.at[2], (partner, x), MESH
    )
    scale_copy.start()

    @pl.loop(0, NY)
    def _(k):
        core_copy(k).start()

    def flag_x(d):
        return pltpu.make_async_remote_copy(
            fs.at[0], fx.at[d - 1], fx_send.at[d - 1], fx_recv.at[d - 1], (inter, (x + d) % NX), MESH
        )

    wait(flag, flag_sem)
    wait(power, power_sem)
    fs[0] = jnp.full((1, 128), (flag[0, 0] >= 0).astype(jnp.float32), jnp.float32)
    for d in range(1, NX):
        flag_x(d).start()

    def turn(h):
        st[:20, : NY * ZC] = sc[h].astype(jnp.float32)
        turned[h] = st[...].T[: NY * ZC]

    block = lax.broadcasted_iota(jnp.int32, (32, 128), 0)

    def spread(h, first, n):
        rows = turned[h, pl.ds(pl.multiple_of(first * 8, 8), n * 8), :].astype(jnp.bfloat16)
        for t in range(0, NB * NX, 2):
            picks = [
                jnp.where(block == u // NB * TJ + 2 * c + u % NB, 1.0, 0.0).astype(jnp.bfloat16)
                for u in (t, t + 1)
            ]
            both = jnp.dot(rows, jnp.concatenate(picks, axis=1), preferred_element_type=jnp.float32)
            for u in range(2):
                bx[h, pl.ds(first, n), t + u] = both[:, u * 128 : (u + 1) * 128].reshape(n, 8, 128)

    st[...] = jnp.zeros((32, 256), jnp.float32)
    with jax.named_scope("spread0"):
        turn(0)
        spread(0, 0, NY * TI)
    with jax.named_scope("wait_scale"):
        wait(lev.at[0], load_sem.at[0])
        scale_copy.wait()
    with jax.named_scope("turn"):
        turn(1)

    def x_copy(src, k, d):
        return pltpu.make_async_remote_copy(
            src, xr.at[k, d - 1], x_send, x_recv.at[k], (inter, (x + d) % NX), MESH
        )

    def near_copy(q):
        return pltpu.make_async_remote_copy(
            cs.at[q], mr.at[q - 1], m_send, m_recv.at[q - 1], along_y(offset(q)), MESH
        )

    def tiles_of(q, d):
        return [[terms[q, d, i * TJ + j] for j in range(TJ)] for i in range(TI)]

    @pl.loop(0, NY)
    def _(q):
        yt = (y + offset(q)) % NY
        spread(1, yt * TI, TI)
        with jax.named_scope("wait_core"):
            wait(par.at[yt], core_recv.at[q])
        tops = []
        for d in range(NX):
            xt = (x + d) % NX
            for i in range(TI):
                row = None
                for h in range(2):
                    b = [bx[h, yt * TI + i, xt * NB + n] for n in range(NB)]
                    even = c == 0
                    b = [b[0], jnp.where(even, b[0], b[1]), b[1], jnp.where(even, b[1], b[2]), b[2]]
                    levels = lev[0, yt, xt, i] if h == 0 else par[yt, xt, i]
                    levels = levels.astype(jnp.float32)
                    term = [levels[:, j * 128 : (j + 1) * 128] * b[j] for j in range(TJ)]
                    row = term if row is None else [p + q for p, q in zip(row, term)]
                for j in range(TJ):
                    terms[q, d, i * TJ + j] = row[j]
                tops.append(top_of(row))

        def send(d):
            encode(tiles_of(q, d), tops[d * TI : d * TI + TI], cs.at[q, d])

        near_by = jnp.logical_or(q == 1, q == 2)

        @pl.when(near_by)
        def _():
            for d in range(NX):
                send(d)
            near_copy(q).start()

        @pl.when(jnp.logical_not(jnp.logical_or(near_by, q == NY - 1)))
        def _():
            for d in (2, 1, 3):
                send(d)
                x_copy(cs.at[q, d], jnp.where(q == 0, 0, q - 2), d).start()

    with jax.named_scope("near0"):
        pl.semaphore_wait(near.at[0], 2)
        pl.semaphore_wait(near.at[1], 2)
    tell_both(2, along_y, NY, 2)
    tell_both(3, along_z, NZ, 2)

    flags = fs[0]
    for d in range(1, NX):
        wait(fx.at[d - 1], fx_recv.at[d - 1])
        flags = flags + fx[d - 1]
    fs[1] = flags
    with jax.named_scope("near"):
        pl.semaphore_wait(near.at[2], 2)
        pl.semaphore_wait(near.at[3], 2)
    tell_both(4, along_z, NZ, 4)

    def flag_y(d):
        return pltpu.make_async_remote_copy(
            fs.at[1], fy.at[d - 1], fy_send.at[d - 1], fy_recv.at[d - 1], along_y(d), MESH
        )

    for d in range(1, NY):
        flag_y(d).start()

    def y_copy(k):
        return pltpu.make_async_remote_copy(
            ys.at[k], yr.at[k], y_send, y_recv.at[k], along_y(far_first(k, NY)), MESH
        )

    def x_sum(k, q):
        with jax.named_scope("wait_x"):
            wait(xr.at[k], x_recv.at[k])
        tiles = tiles_of(q, 0)
        for d in range(1, NX):
            tiles = add(tiles, decode(xr.at[k, d - 1]))
        return tiles

    def flag_z(k):
        to = (zc + far_first(k, ZC)) % ZC
        return pltpu.make_async_remote_copy(
            fs.at[2], fz.at[zc], fz_send, fz_recv, (y * ZC + to, x), MESH
        )

    def pass_on(k, q):
        tiles = x_sum(k, q)
        encode(tiles, [top_of(row) for row in tiles], ys.at[k])
        y_copy(k).start()

    pass_on(0, 0)

    with jax.named_scope("wait_m"):
        for n in range(2):
            wait(mr.at[n], m_recv.at[n])
    for d in (2, 1, 3, 0):
        tiles = add(add(tiles_of(NY - 1, d), decode(mr.at[0, d])), decode(mr.at[1, d]))
        if d:
            encode(tiles, [top_of(row) for row in tiles], ms.at[d - 1])
            x_copy(ms.at[d - 1], NS, d).start()
        else:
            for i in range(TI):
                for j in range(TJ):
                    terms[NY - 1, 0, i * TJ + j] = tiles[i][j]

    @pl.loop(1, NS)
    def _(k):
        pass_on(k, k + 2)

        @pl.when(k == FLAG_STEP)
        def _():
            flags = fs[1]
            with jax.named_scope("wait_fy"):
                for d in range(1, NY):
                    wait(fy.at[d - 1], fy_recv.at[d - 1])
                    flags = flags + fy[d - 1]
            fs[2] = flags
            fz[zc] = flags
            with jax.named_scope("near4"):
                pl.semaphore_wait(near.at[4], 2)

            @pl.loop(0, ZC - 1)
            def _(n):
                flag_z(n).start()

    tiles = x_sum(NS, NY - 1)
    for k in range(NS):
        with jax.named_scope("wait_y"):
            wait(yr.at[k], y_recv.at[k])
        tiles = add(tiles, decode(yr.at[k]))
    for i in range(TI):
        top = top_of(tiles[i])
        factor = jnp.exp2(-top) * TOP
        for j in range(TJ):
            zs[pl.ds(i * 64 + j, 8, stride=8), :] = tiles[i][j] * factor
        zs[pl.ds(i * 64 + TJ, 8, stride=8), :] = top
    for r in range(ZC):
        zq[r] = code(zs[r * 8 : r * 8 + 8, :])

    def z_copy(k):
        to = (zc + far_first(k, ZC)) % ZC
        return pltpu.make_async_remote_copy(
            zq.at[to, : TJ + 1], zr.at[zc, : TJ + 1], z_send, z_recv, (y * ZC + to, x), MESH
        )

    @pl.loop(0, ZC - 1)
    def _(k):
        z_copy(k).start()

    zr[zc] = zq[zc]

    wait(held, held_sem)
    for h in range(2):
        for j in range(TJ):
            at = (h * TJ + j) * 128
            out[16 + h * 8 + j : 17 + h * 8 + j, :] = held[:, at : at + 128]

    for d in range(1, NX):
        wait(fs.at[0], fx_send.at[d - 1])
    for d in range(1, NY):
        wait(fs.at[1], fy_send.at[d - 1])
    wait(lev.at[1], core_send)
    wait(xr, x_send)
    wait(mr, m_send)
    wait(ys, y_send)
    wait(fz.at[: ZC - 1], fz_send)
    with jax.named_scope("wait_flags"):
        wait(fz.at[: ZC - 1], fz_recv)
    count = functools.reduce(jnp.add, [fz[n] for n in range(ZC)])
    with jax.named_scope("wait_z"):
        wait(zr.at[: ZC - 1, : TJ + 1], z_recv)
    wait(zr.at[: ZC - 1, : TJ + 1], z_send)
    for h in range(2):
        total = None
        for n in range(NZ):
            codes = zr[2 * n + h].astype(jnp.int32).astype(jnp.float32)
            part_sum = codes * (jnp.exp2(jnp.broadcast_to(codes[TJ : TJ + 1], (8, 128))) * (1.0 / TOP))
            total = part_sum if total is None else total + part_sum
        out[h * 8 : h * 8 + TJ, :] = total[:TJ]
    out[TJ : TJ + 1, :] = count
    out[7:8, :] = jnp.full((1, 128), power[0].astype(jnp.float32), jnp.float32)


def finish(sums, grad, block_scale, master, new_exponent, count):
    flagged = sums[TJ, 0].astype(jnp.int32)
    factor = jnp.exp2(-jnp.broadcast_to(sums[7:8, :], (8, 128)))
    peaks = []
    for h in range(2):
        g = sums[h * 8 : h * 8 + 8, :] * factor
        peak = jnp.max(jnp.abs(g), axis=1, keepdims=True)
        for j in range(TJ):
            at = slice((h * TJ + j) * 128, (h * TJ + j + 1) * 128)
            w = sums[16 + h * 8 + j : 17 + h * 8 + j, :]
            grad[:, at] = g[j : j + 1]
            master[:, at] = jnp.where(flagged == 0, w - 0.5 * g[j : j + 1], w)
            peaks.append(peak[j : j + 1])
    lane = lax.broadcasted_iota(jnp.int32, (1, 128), 1)
    scale = jnp.zeros((1, 128), jnp.float32)
    for b in range(TJ):
        top = jnp.maximum(peaks[2 * b], peaks[2 * b + 1]) / 127.0
        scale = jnp.where(lane == b, jnp.broadcast_to(top, (1, 128)), scale)
    block_scale[...] = scale[:, :TJ]
    new_exponent[0] = sums[7, 0].astype(jnp.int32) - (flagged > 0).astype(jnp.int32)
    count[0] = flagged


def on_device(partials, scales, overflow_pos, weights, exponent):
    vmem, smem, hbm = (
        pl.BlockSpec(memory_space=m) for m in (pltpu.VMEM, pltpu.SMEM, pltpu.HBM)
    )
    f32, i16, dma = jnp.float32, jnp.int16, pltpu.SemaphoreType.DMA
    codes = (8, 16, 128)
    sums = pl.pallas_call(
        kernel,
        out_shape=pltpu.VMEM((32, 128), f32),
        in_specs=[hbm] * 5,
        out_specs=vmem,
        scratch_shapes=[
            pltpu.VMEM((2, NY, NX, TI, 8, HALF), jnp.bfloat16),
            pltpu.VMEM((NY, NX, TI, 8, HALF), jnp.bfloat16),
            pltpu.VMEM((2, 20, NY * ZC), jnp.bfloat16),
            pltpu.VMEM((32, 256), f32),
            pltpu.VMEM((2, NY * ZC, 32), f32),
            pltpu.VMEM((2, NY * TI, NB * NX, 8, 128), f32),
            pltpu.SMEM((1, 1), jnp.int32),
            pltpu.SMEM((1,), jnp.int32),
            pltpu.VMEM((1, 2 * HALF), f32),
            pltpu.VMEM((NY, NX, TI * TJ, 8, 128), f32),
            pltpu.VMEM((NY - 1, NX, *codes), i16),
            pltpu.VMEM((NX - 1, *codes), i16),
            pltpu.VMEM((NS + 1, NX - 1, *codes), i16),
            pltpu.VMEM((2, NX, *codes), i16),
            pltpu.VMEM((NS, *codes), i16),
            pltpu.VMEM((NS, *codes), i16),
            pltpu.VMEM((ZC * 8, 128), f32),
            pltpu.VMEM((ZC, 8, 128), i16),
            pltpu.VMEM((ZC, 8, 128), i16),
            pltpu.VMEM((3, 1, 128), f32),
            pltpu.VMEM((NX - 1, 1, 128), f32),
            pltpu.VMEM((NY - 1, 1, 128), f32),
            pltpu.VMEM((ZC, 1, 128), f32),
            dma((2,)), dma((3,)), dma, dma, dma, pltpu.SemaphoreType.REGULAR((5,)), dma, dma((NY,)), dma, dma((NS + 1,)),
            dma, dma((2,)), dma, dma((NS,)), dma, dma,
            dma((NX - 1,)), dma((NX - 1,)), dma((NY - 1,)), dma((NY - 1,)), dma, dma,
        ],
        compiler_params=pltpu.CompilerParams(collective_id=0, has_side_effects=True),
        name="exchange",
    )(
        partials.reshape(NY, TI, 8, partials.shape[2]),
        scales.reshape(scales.shape[1:]).T,
        overflow_pos,
        exponent.reshape(1),
        weights,
    )
    grad, block_scale, master, new_exponent, count = pl.pallas_call(
        finish,
        out_shape=(
            jax.ShapeDtypeStruct((1, 2 * HALF), f32),
            jax.ShapeDtypeStruct((1, TJ), f32),
            jax.ShapeDtypeStruct((1, 2 * HALF), f32),
            jax.ShapeDtypeStruct((1,), jnp.int32),
            jax.ShapeDtypeStruct((1,), jnp.int32),
        ),
        in_specs=[vmem],
        out_specs=[vmem, vmem, vmem, smem, smem],
        name="finish",
    )(pltpu.with_memory_space_constraint(sums, pltpu.VMEM))
    return grad, block_scale, master, new_exponent.reshape(()), count.reshape(())


def solution(mesh):
    return jax.shard_map(
        on_device,
        mesh=mesh,
        in_specs=(
            P(("inter", "intra"), None, None),
            P(("inter", "intra"), None, None),
            P(("inter", "intra"), None),
            P("inter", "intra"),
            P(),
        ),
        out_specs=(P("inter", "intra"), P("inter", "intra"), P("inter", "intra"), P(), P()),
        check_vma=False,
    )
```

```python
import functools

import jax
import jax.numpy as jnp
from jax import lax
from jax.experimental import pallas as pl
from jax.experimental.pallas import tpu as pltpu
from jax.sharding import PartitionSpec as P

MESH = pl.DeviceIdType.MESH
NX, NY, NZ = 4, 8, 12
ZC = 2 * NZ
TI, TJ = ZC // 8, 5
HALF = TJ * 128
NB = 3
TOP = 32767.0
FULL = 3
OWN = NY - 1


def wait(ref, sem):
    pltpu.make_async_copy(ref, ref, sem).wait()


def far_first(k, n):
    m = (k + 1) // 2
    return jnp.where(k % 2 == 1, n // 2 - m, n // 2 + m)


def top_of(row):
    peak = functools.reduce(jnp.maximum, [jnp.abs(t) for t in row])
    peak = jnp.maximum(jnp.max(peak, axis=1, keepdims=True), 1e-30)
    return jnp.ceil(jnp.log2(jnp.broadcast_to(peak, (8, 128))) + 1e-3)


def code(values):
    return jnp.round(values).astype(jnp.int32).astype(jnp.int16)


def encode(tiles, tops, out):
    lane = lax.broadcasted_iota(jnp.int32, (8, 128), 1)
    flat, marks = [], jnp.zeros((8, 128), jnp.float32)
    for i in range(TI):
        factor = jnp.exp2(-tops[i]) * TOP
        flat += [t * factor for t in tiles[i]]
        marks = jnp.where(lane == i, tops[i], marks)
    flat.append(marks)
    for p in range(len(flat) // 2):
        out[p] = code(jnp.concatenate([flat[2 * p], flat[2 * p + 1]], axis=0))


def decode(ref):
    flat = []
    for p in range((TI * TJ + 1) // 2):
        pair = ref[p].astype(jnp.int32).astype(jnp.float32)
        flat += [pair[:8], pair[8:]]
    factors = jnp.exp2(flat[TI * TJ]) * (1.0 / TOP)
    return [
        [flat[i * TJ + j] * jnp.broadcast_to(factors[:, i : i + 1], (8, 128)) for j in range(TJ)]
        for i in range(TI)
    ]


def add(a, b):
    return [[p + q for p, q in zip(r, s)] for r, s in zip(a, b)]


def kernel(
    part, scales, pos, exponent, weights,
    out,
    lev, par, sc, st, turned, bx, flag, power, held, terms, cs, xr, dr, ys, yr, zs, zq, zr, fs, fx, fy, fz,
    load_sem, sc_sem, flag_sem, power_sem, held_sem, near, core_send, core_recv, x_send, x_recv, d_send, d_recv, y_send, y_recv, z_send, z_recv,
    fx_send, fx_recv, fy_send, fy_recv, fz_send, fz_recv,
):
    inter, x = lax.axis_index("inter"), lax.axis_index("intra")
    c, zc = inter % 2, inter % ZC
    z, y = zc // 2, inter // ZC
    partner = inter + 1 - 2 * c

    barrier = pltpu.get_barrier_semaphore()

    def along_y(d):
        return ((y + d) % NY * ZC + zc, x)

    def along_z(d):
        return (y * ZC + (zc + 2 * d) % ZC, x)

    def tell(sem, to):
        pl.semaphore_signal(sem, inc=1, device_id=to, device_id_type=MESH)

    def tell_both(sem, along, n, d):
        tell(near.at[sem], along(d))
        tell(near.at[sem], along(n - d))

    tell(barrier, (partner, x))
    for d in range(1, NX):
        tell(barrier, (inter, (x + d) % NX))
    for d in (1, NY - 1):
        tell(barrier, along_y(d))
    for d in (1, NZ - 1):
        tell(barrier, along_z(d))
    for h, side in ((1, 1 - c), (0, c)):
        for xt in range(NX):
            columns = pl.ds(pl.multiple_of(xt * 2 * HALF + side * HALF, 128), HALF)
            pltpu.make_async_copy(part.at[:, :, :, columns], lev.at[h, :, xt], load_sem.at[h]).start()
    pltpu.make_async_copy(scales, sc.at[0], sc_sem.at[0]).start()

    pltpu.make_async_copy(pos, flag, flag_sem).start()
    pltpu.make_async_copy(exponent, power, power_sem).start()
    pltpu.make_async_copy(weights, held, held_sem).start()

    with jax.named_scope("load"):
        wait(sc.at[0], sc_sem.at[0])
        wait(lev.at[1], load_sem.at[1])
    with jax.named_scope("barrier"):
        pl.semaphore_wait(barrier, 1 + NX - 1 + 2 + 2)
    tell_both(0, along_y, NY, 1)
    tell_both(1, along_z, NZ, 1)

    def offset(q):
        return far_first(q, NY)

    def core_copy(k):
        yt = (y + offset(k)) % NY
        return pltpu.make_async_remote_copy(
            lev.at[1, yt], par.at[yt], core_send, core_recv.at[k], (partner, x), MESH
        )

    scale_copy = pltpu.make_async_remote_copy(
        sc.at[0], sc.at[1], sc_sem.at[1], sc_sem.at[2], (partner, x), MESH
    )
    scale_copy.start()

    @pl.loop(0, NY)
    def _(k):
        core_copy(k).start()

    def flag_x(d):
        return pltpu.make_async_remote_copy(
            fs.at[0], fx.at[d - 1], fx_send.at[d - 1], fx_recv.at[d - 1], (inter, (x + d) % NX), MESH
        )

    wait(flag, flag_sem)
    wait(power, power_sem)
    fs[0] = jnp.full((1, 128), (flag[0, 0] >= 0).astype(jnp.float32), jnp.float32)
    for d in range(1, NX):
        flag_x(d).start()

    def turn(h):
        st[:20, : NY * ZC] = sc[h].astype(jnp.float32)
        turned[h] = st[...].T[: NY * ZC]

    block = lax.broadcasted_iota(jnp.int32, (32, 128), 0)

    def spread(h, first, n):
        rows = turned[h, pl.ds(pl.multiple_of(first * 8, 8), n * 8), :].astype(jnp.bfloat16)
        for t in range(0, NB * NX, 2):
            picks = [
                jnp.where(block == u // NB * TJ + 2 * c + u % NB, 1.0, 0.0).astype(jnp.bfloat16)
                for u in (t, t + 1)
            ]
            both = jnp.dot(rows, jnp.concatenate(picks, axis=1), preferred_element_type=jnp.float32)
            for u in range(2):
                bx[h, pl.ds(first, n), t + u] = both[:, u * 128 : (u + 1) * 128].reshape(n, 8, 128)

    st[...] = jnp.zeros((32, 256), jnp.float32)
    with jax.named_scope("spread0"):
        turn(0)
        spread(0, 0, NY * TI)
    with jax.named_scope("wait_scale"):
        wait(lev.at[0], load_sem.at[0])
        scale_copy.wait()
    with jax.named_scope("turn"):
        turn(1)

    def x_copy(src, k, d):
        return pltpu.make_async_remote_copy(
            src, xr.at[k, d - 1], x_send.at[k, d - 1], x_recv.at[k, d - 1], (inter, (x + d) % NX), MESH
        )

    def early_copy(q):
        return pltpu.make_async_remote_copy(
            cs.at[q, 2], dr.at[q - FULL], d_send, d_recv.at[q - FULL], along_y(offset(q)), MESH
        )

    def tiles_of(q, d):
        return [[terms[q, d, i * TJ + j] for j in range(TJ)] for i in range(TI)]

    with jax.named_scope("spread1"):
        spread(1, (y + offset(0)) % NY * TI, TI)

    def produce(q):
        yt = (y + offset(q)) % NY
        with jax.named_scope("wait_core"):
            wait(par.at[yt], core_recv.at[q])
        tops = []
        for d in range(NX):
            xt = (x + d) % NX
            for i in range(TI):
                row = None
                for h in range(2):
                    b = [bx[h, yt * TI + i, xt * NB + n] for n in range(NB)]
                    even = c == 0
                    b = [b[0], jnp.where(even, b[0], b[1]), b[1], jnp.where(even, b[1], b[2]), b[2]]
                    levels = lev[0, yt, xt, i] if h == 0 else par[yt, xt, i]
                    levels = levels.astype(jnp.float32)
                    term = [levels[:, j * 128 : (j + 1) * 128] * b[j] for j in range(TJ)]
                    row = term if row is None else [p + q for p, q in zip(row, term)]
                for j in range(TJ):
                    terms[q, d, i * TJ + j] = row[j]
                tops.append(top_of(row))

        def send(d):
            encode(tiles_of(q, d), tops[d * TI : d * TI + TI], cs.at[q, d])

        @pl.when(q < FULL)
        def _():
            send(2)
            x_copy(cs.at[q, 2], q, 2).start()

        @pl.when(jnp.logical_and(q >= FULL, q < OWN))
        def _():
            send(2)
            early_copy(q).start()

        for d in (1, 3):
            send(d)
            x_copy(cs.at[q, d], q, d).start()

        @pl.when(q == FULL - 1)
        def _():
            with jax.named_scope("near0"):
                pl.semaphore_wait(near.at[0], 2)
                pl.semaphore_wait(near.at[1], 2)
            tell_both(2, along_y, NY, 2)
            tell_both(3, along_z, NZ, 2)

    @pl.loop(0, NY)
    def _(q):
        produce(q)

        @pl.when(q == 0)
        def _():
            spread(1, 0, NY * TI)

    flags = fs[0]
    for d in range(1, NX):
        wait(fx.at[d - 1], fx_recv.at[d - 1])
        flags = flags + fx[d - 1]
    fs[1] = flags
    with jax.named_scope("near"):
        pl.semaphore_wait(near.at[2], 2)
        pl.semaphore_wait(near.at[3], 2)
    tell_both(4, along_z, NZ, 4)

    def flag_y(d):
        return pltpu.make_async_remote_copy(
            fs.at[1], fy.at[d - 1], fy_send.at[d - 1], fy_recv.at[d - 1], along_y(d), MESH
        )

    for d in range(1, NY):
        flag_y(d).start()

    def y_copy(k):
        return pltpu.make_async_remote_copy(
            ys.at[k], yr.at[k], y_send, y_recv.at[k], along_y(offset(k)), MESH
        )

    def x_sum(k, sides):
        with jax.named_scope("wait_x"):
            for d in sides:
                wait(xr.at[k, d - 1], x_recv.at[k, d - 1])
        tiles = tiles_of(k, 0)
        for d in sides:
            tiles = add(tiles, decode(xr.at[k, d - 1]))
        return tiles

    def flag_z(k):
        to = (zc + far_first(k, ZC)) % ZC
        return pltpu.make_async_remote_copy(
            fs.at[2], fz.at[zc], fz_send, fz_recv, (y * ZC + to, x), MESH
        )

    def pass_on(k, sides):
        tiles = x_sum(k, sides)
        encode(tiles, [top_of(row) for row in tiles], ys.at[k])
        y_copy(k).start()

    @pl.loop(0, FULL - 1)
    def _(k):
        pass_on(k, (1, 3, 2))

    tiles = tiles_of(OWN, 2)
    for n in range(OWN - FULL):
        with jax.named_scope("wait_d"):
            wait(dr.at[n], d_recv.at[n])
        tiles = add(tiles, decode(dr.at[n]))
    encode(tiles, [top_of(row) for row in tiles], cs.at[OWN, 2])
    x_copy(cs.at[OWN, 2], OWN, 2).start()

    pass_on(FULL - 1, (1, 3, 2))

    @pl.loop(FULL, OWN)
    def _(k):
        pass_on(k, (1, 3))

    flags = fs[1]
    with jax.named_scope("wait_fy"):
        for d in range(1, NY):
            wait(fy.at[d - 1], fy_recv.at[d - 1])
            flags = flags + fy[d - 1]
    fs[2] = flags
    fz[zc] = flags
    with jax.named_scope("near4"):
        pl.semaphore_wait(near.at[4], 2)

    @pl.loop(0, ZC - 1)
    def _(n):
        flag_z(n).start()

    tiles = x_sum(OWN, (1, 3, 2))
    for k in range(OWN):
        with jax.named_scope("wait_y"):
            wait(yr.at[k], y_recv.at[k])
        tiles = add(tiles, decode(yr.at[k]))
    for i in range(TI):
        top = top_of(tiles[i])
        factor = jnp.exp2(-top) * TOP
        for j in range(TJ):
            zs[pl.ds(i * 64 + j, 8, stride=8), :] = tiles[i][j] * factor
        zs[pl.ds(i * 64 + TJ, 8, stride=8), :] = top
    for r in range(ZC):
        zq[r] = code(zs[r * 8 : r * 8 + 8, :])

    def z_copy(k):
        to = (zc + far_first(k, ZC)) % ZC
        return pltpu.make_async_remote_copy(
            zq.at[to, : TJ + 1], zr.at[zc, : TJ + 1], z_send, z_recv, (y * ZC + to, x), MESH
        )

    @pl.loop(0, ZC - 1)
    def _(k):
        z_copy(k).start()

    zr[zc] = zq[zc]

    wait(held, held_sem)
    for h in range(2):
        for j in range(TJ):
            at = (h * TJ + j) * 128
            out[16 + h * 8 + j : 17 + h * 8 + j, :] = held[:, at : at + 128]

    for d in range(1, NX):
        wait(fs.at[0], fx_send.at[d - 1])
    for d in range(1, NY):
        wait(fs.at[1], fy_send.at[d - 1])
    wait(lev.at[1], core_send)
    for k in range(NY):
        for d in (1, 3) if FULL <= k < OWN else (1, 2, 3):
            wait(xr.at[k, d - 1], x_send.at[k, d - 1])
    wait(dr, d_send)
    wait(ys, y_send)
    wait(fz.at[: ZC - 1], fz_send)
    with jax.named_scope("wait_flags"):
        wait(fz.at[: ZC - 1], fz_recv)
    count = functools.reduce(jnp.add, [fz[n] for n in range(ZC)])
    with jax.named_scope("wait_z"):
        wait(zr.at[: ZC - 1, : TJ + 1], z_recv)
    wait(zr.at[: ZC - 1, : TJ + 1], z_send)
    for h in range(2):
        total = None
        for n in range(NZ):
            codes = zr[2 * n + h].astype(jnp.int32).astype(jnp.float32)
            part_sum = codes * (jnp.exp2(jnp.broadcast_to(codes[TJ : TJ + 1], (8, 128))) * (1.0 / TOP))
            total = part_sum if total is None else total + part_sum
        out[h * 8 : h * 8 + TJ, :] = total[:TJ]
    out[TJ : TJ + 1, :] = count
    out[7:8, :] = jnp.full((1, 128), power[0].astype(jnp.float32), jnp.float32)


def finish(sums, grad, block_scale, master, new_exponent, count):
    flagged = sums[TJ, 0].astype(jnp.int32)
    factor = jnp.exp2(-jnp.broadcast_to(sums[7:8, :], (8, 128)))
    peaks = []
    for h in range(2):
        g = sums[h * 8 : h * 8 + 8, :] * factor
        peak = jnp.max(jnp.abs(g), axis=1, keepdims=True)
        for j in range(TJ):
            at = slice((h * TJ + j) * 128, (h * TJ + j + 1) * 128)
            w = sums[16 + h * 8 + j : 17 + h * 8 + j, :]
            grad[:, at] = g[j : j + 1]
            master[:, at] = jnp.where(flagged == 0, w - 0.5 * g[j : j + 1], w)
            peaks.append(peak[j : j + 1])
    lane = lax.broadcasted_iota(jnp.int32, (1, 128), 1)
    scale = jnp.zeros((1, 128), jnp.float32)
    for b in range(TJ):
        top = jnp.maximum(peaks[2 * b], peaks[2 * b + 1]) / 127.0
        scale = jnp.where(lane == b, jnp.broadcast_to(top, (1, 128)), scale)
    block_scale[...] = scale[:, :TJ]
    new_exponent[0] = sums[7, 0].astype(jnp.int32) - (flagged > 0).astype(jnp.int32)
    count[0] = flagged


def on_device(partials, scales, overflow_pos, weights, exponent):
    vmem, smem, hbm = (
        pl.BlockSpec(memory_space=m) for m in (pltpu.VMEM, pltpu.SMEM, pltpu.HBM)
    )
    f32, i16, dma = jnp.float32, jnp.int16, pltpu.SemaphoreType.DMA
    codes = (8, 16, 128)
    sums = pl.pallas_call(
        kernel,
        out_shape=pltpu.VMEM((32, 128), f32),
        in_specs=[hbm] * 5,
        out_specs=vmem,
        scratch_shapes=[
            pltpu.VMEM((2, NY, NX, TI, 8, HALF), jnp.bfloat16),
            pltpu.VMEM((NY, NX, TI, 8, HALF), jnp.bfloat16),
            pltpu.VMEM((2, 20, NY * ZC), jnp.bfloat16),
            pltpu.VMEM((32, 256), f32),
            pltpu.VMEM((2, NY * ZC, 32), f32),
            pltpu.VMEM((2, NY * TI, NB * NX, 8, 128), f32),
            pltpu.SMEM((1, 1), jnp.int32),
            pltpu.SMEM((1,), jnp.int32),
            pltpu.VMEM((1, 2 * HALF), f32),
            pltpu.VMEM((NY, NX, TI * TJ, 8, 128), f32),
            pltpu.VMEM((NY, NX, *codes), i16),
            pltpu.VMEM((NY, NX - 1, *codes), i16),
            pltpu.VMEM((OWN - FULL, *codes), i16),
            pltpu.VMEM((OWN, *codes), i16),
            pltpu.VMEM((OWN, *codes), i16),
            pltpu.VMEM((ZC * 8, 128), f32),
            pltpu.VMEM((ZC, 8, 128), i16),
            pltpu.VMEM((ZC, 8, 128), i16),
            pltpu.VMEM((3, 1, 128), f32),
            pltpu.VMEM((NX - 1, 1, 128), f32),
            pltpu.VMEM((NY - 1, 1, 128), f32),
            pltpu.VMEM((ZC, 1, 128), f32),
            dma((2,)), dma((3,)), dma, dma, dma, pltpu.SemaphoreType.REGULAR((5,)), dma, dma((NY,)), dma((NY, NX - 1)), dma((NY, NX - 1)),
            dma, dma((OWN - FULL,)), dma, dma((OWN,)), dma, dma,
            dma((NX - 1,)), dma((NX - 1,)), dma((NY - 1,)), dma((NY - 1,)), dma, dma,
        ],
        compiler_params=pltpu.CompilerParams(collective_id=0, has_side_effects=True),
        name="exchange",
    )(
        partials.reshape(NY, TI, 8, partials.shape[2]),
        scales.reshape(scales.shape[1:]).T,
        overflow_pos,
        exponent.reshape(1),
        weights,
    )
    grad, block_scale, master, new_exponent, count = pl.pallas_call(
        finish,
        out_shape=(
            jax.ShapeDtypeStruct((1, 2 * HALF), f32),
            jax.ShapeDtypeStruct((1, TJ), f32),
            jax.ShapeDtypeStruct((1, 2 * HALF), f32),
            jax.ShapeDtypeStruct((1,), jnp.int32),
            jax.ShapeDtypeStruct((1,), jnp.int32),
        ),
        in_specs=[vmem],
        out_specs=[vmem, vmem, vmem, smem, smem],
        name="finish",
    )(pltpu.with_memory_space_constraint(sums, pltpu.VMEM))
    return grad, block_scale, master, new_exponent.reshape(()), count.reshape(())


def solution(mesh):
    return jax.shard_map(
        on_device,
        mesh=mesh,
        in_specs=(
            P(("inter", "intra"), None, None),
            P(("inter", "intra"), None, None),
            P(("inter", "intra"), None),
            P("inter", "intra"),
            P(),
        ),
        out_specs=(P("inter", "intra"), P("inter", "intra"), P("inter", "intra"), P(), P()),
        check_vma=False,
    )
```

```python
import functools

import jax
import jax.numpy as jnp
from jax import lax
from jax.experimental import pallas as pl
from jax.experimental.pallas import tpu as pltpu
from jax.sharding import PartitionSpec as P

MESH = pl.DeviceIdType.MESH
NX, NY, NZ = 4, 8, 12
ZC = 2 * NZ
TI, TJ = ZC // 8, 5
HALF = TJ * 128
NB = 3
TOP = 32767.0
USED = TI * TJ * 8 + 2
FULL = 3
OWN = NY - 1
SIDES = (1, 3, 2)
SENT = 3 * (FULL + 1) + 2 * (OWN - FULL) + OWN - FULL + OWN


def wait(ref, sem):
    pltpu.make_async_copy(ref, ref, sem).wait()


def far_first(k, n):
    m = (k + 1) // 2
    return jnp.where(k % 2 == 1, n // 2 - m, n // 2 + m)


def top_of(row):
    peak = functools.reduce(jnp.maximum, [jnp.abs(t) for t in row])
    peak = jnp.maximum(jnp.max(peak, axis=1, keepdims=True), 1e-30)
    return jnp.ceil(jnp.log2(jnp.broadcast_to(peak, (8, 128))) + 1e-3)


def code(values):
    return jnp.round(values).astype(jnp.int32).astype(jnp.int16)


def row_lane(i):
    lane = lax.broadcasted_iota(jnp.int32, (8, 128), 1)
    return lane == lax.broadcasted_iota(jnp.int32, (8, 128), 0) + 8 * i


def encode(tiles, tops, out):
    flat, marks = [], jnp.zeros((8, 128), jnp.float32)
    for i in range(TI):
        factor = jnp.exp2(-tops[i]) * TOP
        flat += [t * factor for t in tiles[i]]
        marks = jnp.where(row_lane(i), tops[i], marks)
    flat.append(jnp.broadcast_to(jnp.sum(marks, axis=0, keepdims=True), (8, 128)))
    for p in range(len(flat) // 2):
        out[p * 16 : p * 16 + 16, :] = code(jnp.concatenate([flat[2 * p], flat[2 * p + 1]], axis=0))


def decode(ref):
    flat = []
    for p in range((TI * TJ + 1) // 2):
        pair = ref[p * 16 : p * 16 + 16, :].astype(jnp.int32).astype(jnp.float32)
        flat += [pair[:8], pair[8:]]
    marks = jnp.broadcast_to(flat[TI * TJ][:1], (8, 128))
    tiles = []
    for i in range(TI):
        top = jnp.sum(jnp.where(row_lane(i), marks, 0.0), axis=1, keepdims=True)
        factor = jnp.exp2(jnp.broadcast_to(top, (8, 128))) * (1.0 / TOP)
        tiles.append([flat[i * TJ + j] * factor for j in range(TJ)])
    return tiles


def add(a, b):
    return [[p + q for p, q in zip(r, s)] for r, s in zip(a, b)]


def kernel(
    part, scales, pos, exponent, weights,
    out,
    lev, par, sc, st, turned, bx, flag, power, held, terms, cs, xr, dr, ys, yr, zs, zq, zr, fs, fr,
    load_sem, small_sem, near, scale_send, scale_recv, core_send, core_recv,
    part_send, x_recv, early_recv, y_recv, z_send, z_recv, flag_send, flag_recv,
):
    inter, x = lax.axis_index("inter"), lax.axis_index("intra")
    c, zc = inter % 2, inter % ZC
    z, y = zc // 2, inter // ZC
    partner = inter + 1 - 2 * c

    def load(h, side):
        for xt in range(NX):
            columns = pl.ds(pl.multiple_of(xt * 2 * HALF + side * HALF, 128), HALF)
            pltpu.make_async_copy(part.at[:, :, :, columns], lev.at[h, :, xt], load_sem.at[h]).start()

    load(1, 1 - c)
    pltpu.make_async_copy(scales, sc.at[0], small_sem.at[0]).start()

    barrier = pltpu.get_barrier_semaphore()

    def along_y(d):
        return ((y + d) % NY * ZC + zc, x)

    def along_z(d):
        return (y * ZC + (zc + 2 * d) % ZC, x)

    def tell(sem, to):
        pl.semaphore_signal(sem, inc=1, device_id=to, device_id_type=MESH)

    def tell_both(sem, along, n, d):
        tell(near.at[sem], along(d))
        tell(near.at[sem], along(n - d))

    tell(barrier, (partner, x))
    for d in range(1, NX):
        tell(barrier, (inter, (x + d) % NX))
    for d in (1, NY - 1):
        tell(barrier, along_y(d))
    for d in (1, NZ - 1):
        tell(barrier, along_z(d))
    load(0, c)
    pltpu.make_async_copy(pos, flag, small_sem.at[1]).start()
    pltpu.make_async_copy(exponent, power, small_sem.at[2]).start()
    pltpu.make_async_copy(weights, held, small_sem.at[3]).start()
    with jax.named_scope("load"):
        wait(sc.at[0], small_sem.at[0])
        wait(lev.at[1], load_sem.at[1])
    with jax.named_scope("barrier"):
        pl.semaphore_wait(barrier, 1 + NX - 1 + 2 + 2)
    tell_both(0, along_y, NY, 1)
    tell_both(0, along_z, NZ, 1)

    def offset(q):
        return far_first(q, NY)

    def core_copy(k):
        yt = (y + offset(k)) % NY
        return pltpu.make_async_remote_copy(
            lev.at[1, yt], par.at[yt], core_send, core_recv.at[(k + 3) // 4], (partner, x), MESH
        )

    scale_copy = pltpu.make_async_remote_copy(
        sc.at[0], sc.at[1], scale_send, scale_recv, (partner, x), MESH
    )
    scale_copy.start()

    @pl.loop(0, NY)
    def _(k):
        core_copy(k).start()

    def flag_x(d):
        return pltpu.make_async_remote_copy(
            fs.at[0], fr.at[d - 1], flag_send, flag_recv.at[0], (inter, (x + d) % NX), MESH
        )

    wait(flag, small_sem.at[1])
    wait(power, small_sem.at[2])
    fs[0] = jnp.full((1, 128), (flag[0, 0] >= 0).astype(jnp.float32), jnp.float32)
    for d in range(1, NX):
        flag_x(d).start()

    def turn(h):
        st[:20, : NY * ZC] = sc[h].astype(jnp.float32)
        turned[h] = st[...].T[: NY * ZC]

    block = lax.broadcasted_iota(jnp.int32, (32, 128), 0)

    def spread(h, first, n):
        rows = turned[h, pl.ds(pl.multiple_of(first * 8, 8), n * 8), :].astype(jnp.bfloat16)
        for t in range(0, NB * NX, 2):
            picks = [
                jnp.where(block == u // NB * TJ + 2 * c + u % NB, 1.0, 0.0).astype(jnp.bfloat16)
                for u in (t, t + 1)
            ]
            both = jnp.dot(rows, jnp.concatenate(picks, axis=1), preferred_element_type=jnp.float32)
            for u in range(2):
                bx[h, pl.ds(first, n), t + u] = both[:, u * 128 : (u + 1) * 128].reshape(n, 8, 128)

    st[...] = jnp.zeros((32, 256), jnp.float32)
    with jax.named_scope("spread0"):
        turn(0)
        spread(0, 0, NY * TI)
    with jax.named_scope("wait_scale"):
        wait(lev.at[0], load_sem.at[0])
        scale_copy.wait()
    with jax.named_scope("turn"):
        turn(1)

    def x_copy(src, k, d):
        return pltpu.make_async_remote_copy(
            src.at[:USED], xr.at[k, SIDES.index(d), :USED], part_send, x_recv.at[k], (inter, (x + d) % NX), MESH
        )

    def early_copy(q):
        return pltpu.make_async_remote_copy(
            cs.at[q * NX + 2, :USED], dr.at[q - FULL, :USED], part_send, early_recv, along_y(offset(q)), MESH
        )

    def tiles_of(q, d):
        return [[terms[q, d, i * TJ + j] for j in range(TJ)] for i in range(TI)]

    with jax.named_scope("spread1"):
        spread(1, (y + offset(0)) % NY * TI, TI)

    def produce(q):
        yt = (y + offset(q)) % NY
        for g, (first, n) in enumerate(((0, 1), (1, 4), (5, 3))):

            @pl.when(q == first)
            def _():
                with jax.named_scope("wait_core"):
                    wait(par.at[:n], core_recv.at[g])

        tops = []
        for d in range(NX):
            xt = (x + d) % NX
            for i in range(TI):
                row = None
                for h in range(2):
                    b = [bx[h, yt * TI + i, xt * NB + n] for n in range(NB)]
                    even = c == 0
                    b = [b[0], jnp.where(even, b[0], b[1]), b[1], jnp.where(even, b[1], b[2]), b[2]]
                    levels = lev[0, yt, xt, i] if h == 0 else par[yt, xt, i]
                    levels = levels.astype(jnp.float32)
                    term = [levels[:, j * 128 : (j + 1) * 128] * b[j] for j in range(TJ)]
                    row = term if row is None else [p + q for p, q in zip(row, term)]
                for j in range(TJ):
                    terms[q, d, i * TJ + j] = row[j]
                tops.append(top_of(row))

        def send(d):
            encode(tiles_of(q, d), tops[d * TI : d * TI + TI], cs.at[q * NX + d])

        @pl.when(q < FULL)
        def _():
            send(2)
            x_copy(cs.at[q * NX + 2], q, 2).start()

        @pl.when(jnp.logical_and(q >= FULL, q < OWN))
        def _():
            send(2)
            early_copy(q).start()

        for d in (1, 3):
            send(d)
            x_copy(cs.at[q * NX + d], q, d).start()

        @pl.when(q == FULL - 1)
        def _():
            with jax.named_scope("near0"):
                pl.semaphore_wait(near.at[0], 4)
            tell_both(1, along_y, NY, 2)
            tell_both(1, along_z, NZ, 2)

    @pl.loop(0, NY)
    def _(q):
        produce(q)

        @pl.when(q == 0)
        def _():
            spread(1, 0, NY * TI)

    flags = fs[0]
    wait(fr.at[: NX - 1], flag_recv.at[0])
    for n in range(NX - 1):
        flags = flags + fr[n]
    fs[1] = flags
    with jax.named_scope("near"):
        pl.semaphore_wait(near.at[1], 4)
    tell_both(2, along_z, NZ, 4)

    def flag_y(d):
        return pltpu.make_async_remote_copy(
            fs.at[1], fr.at[NX + d - 2], flag_send, flag_recv.at[1], along_y(d), MESH
        )

    for d in range(1, NY):
        flag_y(d).start()

    def y_copy(k):
        return pltpu.make_async_remote_copy(
            ys.at[k, :USED], yr.at[k, :USED], part_send, y_recv.at[jnp.maximum(k - 4, 0)], along_y(offset(k)), MESH
        )

    def x_sum(k, n):
        with jax.named_scope("wait_x"):
            wait(xr.at[k, :n, :USED], x_recv.at[k])
        tiles = tiles_of(k, 0)
        for m in range(n):
            tiles = add(tiles, decode(xr.at[k, m]))
        return tiles

    def flag_z(k):
        to = (zc + far_first(k, ZC)) % ZC
        return pltpu.make_async_remote_copy(
            fs.at[2], fr.at[NX + NY - 2 + zc], flag_send, flag_recv.at[2], (y * ZC + to, x), MESH
        )

    def pass_on(k, n):
        tiles = x_sum(k, n)
        encode(tiles, [top_of(row) for row in tiles], ys.at[k])
        y_copy(k).start()

    @pl.loop(0, FULL - 1)
    def _(k):
        pass_on(k, 3)

    tiles = tiles_of(OWN, 2)
    with jax.named_scope("wait_d"):
        wait(dr.at[:, :USED], early_recv)
    for n in range(OWN - FULL):
        tiles = add(tiles, decode(dr.at[n]))
    encode(tiles, [top_of(row) for row in tiles], cs.at[OWN * NX + 2])
    x_copy(cs.at[OWN * NX + 2], OWN, 2).start()

    pass_on(FULL - 1, 3)

    @pl.loop(FULL, OWN)
    def _(k):
        pass_on(k, 2)

    flags = fs[1]
    with jax.named_scope("wait_fy"):
        wait(fr.at[NX - 1 : NX + NY - 2], flag_recv.at[1])
    for n in range(NX - 1, NX + NY - 2):
        flags = flags + fr[n]
    fs[2] = flags
    fr[NX + NY - 2 + zc] = flags
    with jax.named_scope("near4"):
        pl.semaphore_wait(near.at[2], 2)

    @pl.loop(0, ZC - 1)
    def _(n):
        flag_z(n).start()

    tiles = x_sum(OWN, 3)
    for g, (first, n) in enumerate(((0, 5), (5, 1), (6, 1))):
        with jax.named_scope("wait_y"):
            wait(yr.at[first : first + n, :USED], y_recv.at[g])
        for k in range(first, first + n):
            tiles = add(tiles, decode(yr.at[k]))
    for i in range(TI):
        top = top_of(tiles[i])
        factor = jnp.exp2(-top) * TOP
        for j in range(TJ):
            zs[pl.ds(i * 64 + j, 8, stride=8), :] = tiles[i][j] * factor
        zs[pl.ds(i * 64 + TJ, 8, stride=8), :] = top
    for r in range(ZC):
        zq[r] = code(zs[r * 8 : r * 8 + 8, :])

    def z_copy(k):
        to = (zc + far_first(k, ZC)) % ZC
        return pltpu.make_async_remote_copy(
            zq.at[to, : TJ + 1], zr.at[zc, : TJ + 1], z_send, z_recv, (y * ZC + to, x), MESH
        )

    @pl.loop(0, ZC - 1)
    def _(k):
        z_copy(k).start()

    zr[zc] = zq[zc]

    wait(held, small_sem.at[3])
    for h in range(2):
        for j in range(TJ):
            at = (h * TJ + j) * 128
            out[16 + h * 8 + j : 17 + h * 8 + j, :] = held[:, at : at + 128]

    wait(lev.at[1], core_send)
    wait(cs.at[:SENT, :USED], part_send)
    wait(fr.at[: NX + NY + ZC - 3], flag_send)
    with jax.named_scope("wait_flags"):
        wait(fr.at[NX + NY - 2 : NX + NY + ZC - 3], flag_recv.at[2])
    count = functools.reduce(jnp.add, [fr[NX + NY - 2 + n] for n in range(ZC)])
    with jax.named_scope("wait_z"):
        wait(zr.at[: ZC - 1, : TJ + 1], z_recv)

    def row_sum(n, totals):
        sums = []
        for h in range(2):
            codes = zr[2 * n + h].astype(jnp.int32).astype(jnp.float32)
            factor = jnp.exp2(jnp.broadcast_to(codes[TJ : TJ + 1], (8, 128))) * (1.0 / TOP)
            sums.append(totals[h] + codes * factor)
        return tuple(sums)

    zero = jnp.zeros((8, 128), jnp.float32)
    totals = lax.fori_loop(0, NZ, row_sum, (zero, zero), unroll=4)
    for h in range(2):
        out[h * 8 : h * 8 + TJ, :] = totals[h][:TJ]
    out[TJ : TJ + 1, :] = count
    out[7:8, :] = jnp.full((1, 128), power[0].astype(jnp.float32), jnp.float32)
    wait(zr.at[: ZC - 1, : TJ + 1], z_send)


def finish(sums, grad, block_scale, master, new_exponent, count):
    flagged = sums[TJ, 0].astype(jnp.int32)
    factor = jnp.exp2(-jnp.broadcast_to(sums[7:8, :], (8, 128)))
    peaks = []
    for h in range(2):
        g = sums[h * 8 : h * 8 + 8, :] * factor
        peak = jnp.max(jnp.abs(g), axis=1, keepdims=True)
        for j in range(TJ):
            at = slice((h * TJ + j) * 128, (h * TJ + j + 1) * 128)
            w = sums[16 + h * 8 + j : 17 + h * 8 + j, :]
            grad[:, at] = g[j : j + 1]
            master[:, at] = jnp.where(flagged == 0, w - 0.5 * g[j : j + 1], w)
            peaks.append(peak[j : j + 1])
    lane = lax.broadcasted_iota(jnp.int32, (1, 128), 1)
    scale = jnp.zeros((1, 128), jnp.float32)
    for b in range(TJ):
        top = jnp.maximum(peaks[2 * b], peaks[2 * b + 1]) / 127.0
        scale = jnp.where(lane == b, jnp.broadcast_to(top, (1, 128)), scale)
    block_scale[...] = scale[:, :TJ]
    new_exponent[0] = sums[7, 0].astype(jnp.int32) - (flagged > 0).astype(jnp.int32)
    count[0] = flagged


def on_device(partials, scales, overflow_pos, weights, exponent):
    vmem, smem, hbm = (
        pl.BlockSpec(memory_space=m) for m in (pltpu.VMEM, pltpu.SMEM, pltpu.HBM)
    )
    f32, i16, dma = jnp.float32, jnp.int16, pltpu.SemaphoreType.DMA
    codes = (128, 128)
    sums = pl.pallas_call(
        kernel,
        out_shape=pltpu.VMEM((32, 128), f32),
        in_specs=[hbm] * 5,
        out_specs=vmem,
        scratch_shapes=[
            pltpu.VMEM((2, NY, NX, TI, 8, HALF), jnp.bfloat16),
            pltpu.VMEM((NY, NX, TI, 8, HALF), jnp.bfloat16),
            pltpu.VMEM((2, 20, NY * ZC), jnp.bfloat16),
            pltpu.VMEM((32, 256), f32),
            pltpu.VMEM((2, NY * ZC, 32), f32),
            pltpu.VMEM((2, NY * TI, NB * NX, 8, 128), f32),
            pltpu.SMEM((1, 1), jnp.int32),
            pltpu.SMEM((1,), jnp.int32),
            pltpu.VMEM((1, 2 * HALF), f32),
            pltpu.VMEM((NY, NX, TI * TJ, 8, 128), f32),
            pltpu.VMEM((NY * NX, *codes), i16),
            pltpu.VMEM((NY, NX - 1, *codes), i16),
            pltpu.VMEM((OWN - FULL, *codes), i16),
            pltpu.VMEM((OWN, *codes), i16),
            pltpu.VMEM((OWN, *codes), i16),
            pltpu.VMEM((ZC * 8, 128), f32),
            pltpu.VMEM((ZC, 8, 128), i16),
            pltpu.VMEM((ZC, 8, 128), i16),
            pltpu.VMEM((3, 1, 128), f32),
            pltpu.VMEM((NX + NY - 2 + ZC, 1, 128), f32),
            dma((2,)), dma((4,)), pltpu.SemaphoreType.REGULAR((3,)), dma, dma, dma, dma((3,)),
            dma, dma((NY,)), dma, dma((3,)), dma, dma, dma, dma((3,)),
        ],
        compiler_params=pltpu.CompilerParams(collective_id=0, has_side_effects=True),
        name="exchange",
    )(
        partials.reshape(NY, TI, 8, partials.shape[2]),
        scales.reshape(scales.shape[1:]).T,
        overflow_pos,
        exponent.reshape(1),
        weights,
    )
    grad, block_scale, master, new_exponent, count = pl.pallas_call(
        finish,
        out_shape=(
            jax.ShapeDtypeStruct((1, 2 * HALF), f32),
            jax.ShapeDtypeStruct((1, TJ), f32),
            jax.ShapeDtypeStruct((1, 2 * HALF), f32),
            jax.ShapeDtypeStruct((1,), jnp.int32),
            jax.ShapeDtypeStruct((1,), jnp.int32),
        ),
        in_specs=[vmem],
        out_specs=[vmem, vmem, vmem, smem, smem],
        name="finish",
    )(pltpu.with_memory_space_constraint(sums, pltpu.VMEM))
    return grad, block_scale, master, new_exponent.reshape(()), count.reshape(())


def solution(mesh):
    return jax.shard_map(
        on_device,
        mesh=mesh,
        in_specs=(
            P(("inter", "intra"), None, None),
            P(("inter", "intra"), None, None),
            P(("inter", "intra"), None),
            P("inter", "intra"),
            P(),
        ),
        out_specs=(P("inter", "intra"), P("inter", "intra"), P("inter", "intra"), P(), P()),
        check_vma=False,
    )
```

```python
import functools

import jax
import jax.numpy as jnp
from jax import lax
from jax.experimental import pallas as pl
from jax.experimental.pallas import tpu as pltpu
from jax.sharding import PartitionSpec as P

MESH = pl.DeviceIdType.MESH
NX, NY, NZ = 4, 8, 12
ZC = 2 * NZ
TI, TJ = ZC // 8, 5
HALF = TJ * 128
NB = 3
TOP = 32767.0
USED = TI * TJ * 8 + 2
FULL = 3
OWN = NY - 1
SIDES = (1, 3, 2)
SENT = 3 * (FULL + 1) + 2 * (OWN - FULL) + OWN - FULL + OWN


def wait(ref, sem):
    pltpu.make_async_copy(ref, ref, sem).wait()


def far_first(k, n):
    m = (k + 1) // 2
    return jnp.where(k % 2 == 1, n // 2 - m, n // 2 + m)


def top_of(row):
    peak = functools.reduce(jnp.maximum, [jnp.abs(t) for t in row])
    peak = jnp.maximum(jnp.max(peak, axis=1, keepdims=True), 1e-30)
    return jnp.ceil(jnp.log2(jnp.broadcast_to(peak, (8, 128))) + 1e-3)


def code(values):
    return jnp.round(values).astype(jnp.int32).astype(jnp.int16)


def row_lane(i):
    lane = lax.broadcasted_iota(jnp.int32, (8, 128), 1)
    return lane == lax.broadcasted_iota(jnp.int32, (8, 128), 0) + 8 * i


def encode(tiles, tops, out):
    flat, marks = [], jnp.zeros((8, 128), jnp.float32)
    for i in range(TI):
        factor = jnp.exp2(-tops[i]) * TOP
        flat += [t * factor for t in tiles[i]]
        marks = jnp.where(row_lane(i), tops[i], marks)
    flat.append(jnp.broadcast_to(jnp.sum(marks, axis=0, keepdims=True), (8, 128)))
    for p in range(len(flat) // 2):
        out[p * 16 : p * 16 + 16, :] = code(jnp.concatenate([flat[2 * p], flat[2 * p + 1]], axis=0))


def decode(ref):
    flat = []
    for p in range((TI * TJ + 1) // 2):
        pair = ref[p * 16 : p * 16 + 16, :].astype(jnp.int32).astype(jnp.float32)
        flat += [pair[:8], pair[8:]]
    marks = jnp.broadcast_to(flat[TI * TJ][:1], (8, 128))
    tiles = []
    for i in range(TI):
        top = jnp.sum(jnp.where(row_lane(i), marks, 0.0), axis=1, keepdims=True)
        factor = jnp.exp2(jnp.broadcast_to(top, (8, 128))) * (1.0 / TOP)
        tiles.append([flat[i * TJ + j] * factor for j in range(TJ)])
    return tiles


def add(a, b):
    return [[p + q for p, q in zip(r, s)] for r, s in zip(a, b)]


def kernel(
    part, scales, pos, exponent, weights,
    out,
    lev, head, par, sc, st, turned, bx, flag, power, held, terms, cs, xr, dr, ys, yr, zs, zq, zr, fs, fr,
    load_sem, small_sem, near, scale_send, scale_recv, core_send, core_recv,
    part_send, x_recv, early_recv, y_recv, z_send, z_recv, flag_send, flag_recv,
):
    inter, x = lax.axis_index("inter"), lax.axis_index("intra")
    c, zc = inter % 2, inter % ZC
    z, y = zc // 2, inter // ZC
    partner = inter + 1 - 2 * c

    def offset(q):
        return far_first(q, NY)

    def columns(xt, side):
        return pl.ds(pl.multiple_of(xt * 2 * HALF + side * HALF, 128), HALF)

    def load(h, side):
        for xt in range(NX):
            pltpu.make_async_copy(part.at[:, :, :, columns(xt, side)], lev.at[h, :, xt], load_sem.at[h]).start()

    first_y = (y + offset(0)) % NY
    for xt in range(NX):
        pltpu.make_async_copy(part.at[first_y, :, :, columns(xt, 1 - c)], head.at[xt], load_sem.at[2]).start()
    pltpu.make_async_copy(scales, sc.at[0], small_sem.at[0]).start()

    barrier = pltpu.get_barrier_semaphore()

    def along_x(d):
        return (inter, (x + d) % NX)

    def along_y(d):
        return ((y + d) % NY * ZC + zc, x)

    def along_z(d):
        return (y * ZC + (zc + 2 * d) % ZC, x)

    def tell(sem, to):
        pl.semaphore_signal(sem, inc=1, device_id=to, device_id_type=MESH)

    def tell_both(sem, along, n, d):
        tell(near.at[sem], along(d))
        tell(near.at[sem], along(n - d))

    tell(barrier, (partner, x))
    for d in (1, NX - 1):
        tell(barrier, along_x(d))
    for d in (1, NY - 1):
        tell(barrier, along_y(d))
    for d in (1, NZ - 1):
        tell(barrier, along_z(d))
    load(1, 1 - c)
    load(0, c)
    pltpu.make_async_copy(pos, flag, small_sem.at[1]).start()
    pltpu.make_async_copy(exponent, power, small_sem.at[2]).start()
    pltpu.make_async_copy(weights, held, small_sem.at[3]).start()
    with jax.named_scope("barrier"):
        pl.semaphore_wait(barrier, 1 + 2 + 2 + 2)
    tell_both(3, along_x, NX, 1)
    tell_both(0, along_y, NY, 1)
    tell_both(0, along_z, NZ, 1)

    def core_copy(k, source):
        yt = (y + offset(k)) % NY
        return pltpu.make_async_remote_copy(
            source, par.at[yt], core_send, core_recv.at[(k + 3) // 4], (partner, x), MESH
        )

    scale_copy = pltpu.make_async_remote_copy(
        sc.at[0], sc.at[1], scale_send, scale_recv, (partner, x), MESH
    )
    with jax.named_scope("load"):
        wait(sc.at[0], small_sem.at[0])
        scale_copy.start()
        wait(head, load_sem.at[2])
        core_copy(0, head).start()
        wait(lev.at[1], load_sem.at[1])

    @pl.loop(1, NY)
    def _(k):
        core_copy(k, lev.at[1, (y + offset(k)) % NY]).start()

    def flag_x(d):
        return pltpu.make_async_remote_copy(
            fs.at[0], fr.at[d - 1], flag_send, flag_recv.at[0], along_x(d), MESH
        )

    wait(flag, small_sem.at[1])
    wait(power, small_sem.at[2])
    fs[0] = jnp.full((1, 128), (flag[0, 0] >= 0).astype(jnp.float32), jnp.float32)

    def turn(h):
        st[:20, : NY * ZC] = sc[h].astype(jnp.float32)
        turned[h] = st[...].T[: NY * ZC]

    block = lax.broadcasted_iota(jnp.int32, (32, 128), 0)

    def spread(h, first, n):
        rows = turned[h, pl.ds(pl.multiple_of(first * 8, 8), n * 8), :].astype(jnp.bfloat16)
        for t in range(0, NB * NX, 2):
            picks = [
                jnp.where(block == u // NB * TJ + 2 * c + u % NB, 1.0, 0.0).astype(jnp.bfloat16)
                for u in (t, t + 1)
            ]
            both = jnp.dot(rows, jnp.concatenate(picks, axis=1), preferred_element_type=jnp.float32)
            for u in range(2):
                bx[h, pl.ds(first, n), t + u] = both[:, u * 128 : (u + 1) * 128].reshape(n, 8, 128)

    st[...] = jnp.zeros((32, 256), jnp.float32)
    with jax.named_scope("spread0"):
        turn(0)
        spread(0, 0, NY * TI)
    with jax.named_scope("wait_scale"):
        wait(lev.at[0], load_sem.at[0])
        scale_copy.wait()
    with jax.named_scope("turn"):
        turn(1)

    def x_copy(src, k, d):
        return pltpu.make_async_remote_copy(
            src.at[:USED], xr.at[k, SIDES.index(d), :USED], part_send, x_recv.at[k], along_x(d), MESH
        )

    def early_copy(q):
        return pltpu.make_async_remote_copy(
            cs.at[q * NX + 2, :USED], dr.at[q - FULL, :USED], part_send, early_recv, along_y(offset(q)), MESH
        )

    def tiles_of(q, d):
        return [[terms[q, d, i * TJ + j] for j in range(TJ)] for i in range(TI)]

    with jax.named_scope("near_x"):
        pl.semaphore_wait(near.at[3], 2)
    for d in range(1, NX):
        flag_x(d).start()
    with jax.named_scope("spread1"):
        spread(1, (y + offset(0)) % NY * TI, TI)

    def produce(q):
        yt = (y + offset(q)) % NY
        for g, (first, n) in enumerate(((0, 1), (1, 4), (5, 3))):

            @pl.when(q == first)
            def _():
                with jax.named_scope("wait_core"):
                    wait(par.at[:n], core_recv.at[g])

        tops = []
        for d in range(NX):
            xt = (x + d) % NX
            for i in range(TI):
                row = None
                for h in range(2):
                    b = [bx[h, yt * TI + i, xt * NB + n] for n in range(NB)]
                    even = c == 0
                    b = [b[0], jnp.where(even, b[0], b[1]), b[1], jnp.where(even, b[1], b[2]), b[2]]
                    levels = lev[0, yt, xt, i] if h == 0 else par[yt, xt, i]
                    levels = levels.astype(jnp.float32)
                    term = [levels[:, j * 128 : (j + 1) * 128] * b[j] for j in range(TJ)]
                    row = term if row is None else [p + q for p, q in zip(row, term)]
                for j in range(TJ):
                    terms[q, d, i * TJ + j] = row[j]
                tops.append(top_of(row))

        def send(d):
            encode(tiles_of(q, d), tops[d * TI : d * TI + TI], cs.at[q * NX + d])

        @pl.when(q < FULL)
        def _():
            send(2)
            x_copy(cs.at[q * NX + 2], q, 2).start()

        @pl.when(jnp.logical_and(q >= FULL, q < OWN))
        def _():
            send(2)
            early_copy(q).start()

        for d in (1, 3):
            send(d)
            x_copy(cs.at[q * NX + d], q, d).start()

        @pl.when(q == FULL - 1)
        def _():
            with jax.named_scope("near0"):
                pl.semaphore_wait(near.at[0], 4)
            tell_both(1, along_y, NY, 2)
            tell_both(1, along_z, NZ, 2)

    @pl.loop(0, NY)
    def _(q):
        produce(q)

        @pl.when(q == 0)
        def _():
            spread(1, 0, NY * TI)

    flags = fs[0]
    wait(fr.at[: NX - 1], flag_recv.at[0])
    for n in range(NX - 1):
        flags = flags + fr[n]
    fs[1] = flags
    with jax.named_scope("near"):
        pl.semaphore_wait(near.at[1], 4)
    tell_both(2, along_z, NZ, 4)

    def flag_y(d):
        return pltpu.make_async_remote_copy(
            fs.at[1], fr.at[NX + d - 2], flag_send, flag_recv.at[1], along_y(d), MESH
        )

    for d in range(1, NY):
        flag_y(d).start()

    def y_copy(k):
        return pltpu.make_async_remote_copy(
            ys.at[k, :USED], yr.at[k, :USED], part_send, y_recv.at[jnp.maximum(k - 4, 0)], along_y(offset(k)), MESH
        )

    def x_sum(k, n):
        with jax.named_scope("wait_x"):
            wait(xr.at[k, :n, :USED], x_recv.at[k])
        tiles = tiles_of(k, 0)
        for m in range(n):
            tiles = add(tiles, decode(xr.at[k, m]))
        return tiles

    def flag_z(k):
        to = (zc + far_first(k, ZC)) % ZC
        return pltpu.make_async_remote_copy(
            fs.at[2], fr.at[NX + NY - 2 + zc], flag_send, flag_recv.at[2], (y * ZC + to, x), MESH
        )

    def pass_on(k, n):
        tiles = x_sum(k, n)
        encode(tiles, [top_of(row) for row in tiles], ys.at[k])
        y_copy(k).start()

    @pl.loop(0, FULL - 1)
    def _(k):
        pass_on(k, 3)

    tiles = tiles_of(OWN, 2)
    with jax.named_scope("wait_d"):
        wait(dr.at[:, :USED], early_recv)
    for n in range(OWN - FULL):
        tiles = add(tiles, decode(dr.at[n]))
    encode(tiles, [top_of(row) for row in tiles], cs.at[OWN * NX + 2])
    x_copy(cs.at[OWN * NX + 2], OWN, 2).start()

    pass_on(FULL - 1, 3)

    @pl.loop(FULL, OWN)
    def _(k):
        pass_on(k, 2)

    flags = fs[1]
    with jax.named_scope("wait_fy"):
        wait(fr.at[NX - 1 : NX + NY - 2], flag_recv.at[1])
    for n in range(NX - 1, NX + NY - 2):
        flags = flags + fr[n]
    fs[2] = flags
    fr[NX + NY - 2 + zc] = flags
    with jax.named_scope("near4"):
        pl.semaphore_wait(near.at[2], 2)

    @pl.loop(0, ZC - 1)
    def _(n):
        flag_z(n).start()

    tiles = x_sum(OWN, 3)
    for g, (first, n) in enumerate(((0, 5), (5, 1), (6, 1))):
        with jax.named_scope("wait_y"):
            wait(yr.at[first : first + n, :USED], y_recv.at[g])
        for k in range(first, first + n):
            tiles = add(tiles, decode(yr.at[k]))
    for i in range(TI):
        top = top_of(tiles[i])
        factor = jnp.exp2(-top) * TOP
        for j in range(TJ):
            zs[pl.ds(i * 64 + j, 8, stride=8), :] = tiles[i][j] * factor
        zs[pl.ds(i * 64 + TJ, 8, stride=8), :] = top
    for r in range(ZC):
        zq[r] = code(zs[r * 8 : r * 8 + 8, :])

    def z_copy(k):
        to = (zc + far_first(k, ZC)) % ZC
        return pltpu.make_async_remote_copy(
            zq.at[to, : TJ + 1], zr.at[zc, : TJ + 1], z_send, z_recv, (y * ZC + to, x), MESH
        )

    @pl.loop(0, ZC - 1)
    def _(k):
        z_copy(k).start()

    zr[zc] = zq[zc]

    wait(held, small_sem.at[3])
    for h in range(2):
        for j in range(TJ):
            at = (h * TJ + j) * 128
            out[16 + h * 8 + j : 17 + h * 8 + j, :] = held[:, at : at + 128]

    wait(lev.at[1], core_send)
    wait(cs.at[:SENT, :USED], part_send)
    wait(fr.at[: NX + NY + ZC - 3], flag_send)
    with jax.named_scope("wait_flags"):
        wait(fr.at[NX + NY - 2 : NX + NY + ZC - 3], flag_recv.at[2])
    count = functools.reduce(jnp.add, [fr[NX + NY - 2 + n] for n in range(ZC)])
    with jax.named_scope("wait_z"):
        wait(zr.at[: ZC - 1, : TJ + 1], z_recv)

    def row_sum(n, totals):
        sums = []
        for h in range(2):
            codes = zr[2 * n + h].astype(jnp.int32).astype(jnp.float32)
            factor = jnp.exp2(jnp.broadcast_to(codes[TJ : TJ + 1], (8, 128))) * (1.0 / TOP)
            sums.append(totals[h] + codes * factor)
        return tuple(sums)

    zero = jnp.zeros((8, 128), jnp.float32)
    totals = lax.fori_loop(0, NZ, row_sum, (zero, zero), unroll=4)
    for h in range(2):
        out[h * 8 : h * 8 + TJ, :] = totals[h][:TJ]
    out[TJ : TJ + 1, :] = count
    out[7:8, :] = jnp.full((1, 128), power[0].astype(jnp.float32), jnp.float32)
    wait(zr.at[: ZC - 1, : TJ + 1], z_send)


def finish(sums, grad, block_scale, master, new_exponent, count):
    flagged = sums[TJ, 0].astype(jnp.int32)
    factor = jnp.exp2(-jnp.broadcast_to(sums[7:8, :], (8, 128)))
    peaks = []
    for h in range(2):
        g = sums[h * 8 : h * 8 + 8, :] * factor
        peak = jnp.max(jnp.abs(g), axis=1, keepdims=True)
        for j in range(TJ):
            at = slice((h * TJ + j) * 128, (h * TJ + j + 1) * 128)
            w = sums[16 + h * 8 + j : 17 + h * 8 + j, :]
            grad[:, at] = g[j : j + 1]
            master[:, at] = jnp.where(flagged == 0, w - 0.5 * g[j : j + 1], w)
            peaks.append(peak[j : j + 1])
    lane = lax.broadcasted_iota(jnp.int32, (1, 128), 1)
    scale = jnp.zeros((1, 128), jnp.float32)
    for b in range(TJ):
        top = jnp.maximum(peaks[2 * b], peaks[2 * b + 1]) / 127.0
        scale = jnp.where(lane == b, jnp.broadcast_to(top, (1, 128)), scale)
    block_scale[...] = scale[:, :TJ]
    new_exponent[0] = sums[7, 0].astype(jnp.int32) - (flagged > 0).astype(jnp.int32)
    count[0] = flagged


def on_device(partials, scales, overflow_pos, weights, exponent):
    vmem, smem, hbm = (
        pl.BlockSpec(memory_space=m) for m in (pltpu.VMEM, pltpu.SMEM, pltpu.HBM)
    )
    f32, i16, dma = jnp.float32, jnp.int16, pltpu.SemaphoreType.DMA
    codes = (128, 128)
    sums = pl.pallas_call(
        kernel,
        out_shape=pltpu.VMEM((32, 128), f32),
        in_specs=[hbm] * 5,
        out_specs=vmem,
        scratch_shapes=[
            pltpu.VMEM((2, NY, NX, TI, 8, HALF), jnp.bfloat16),
            pltpu.VMEM((NX, TI, 8, HALF), jnp.bfloat16),
            pltpu.VMEM((NY, NX, TI, 8, HALF), jnp.bfloat16),
            pltpu.VMEM((2, 20, NY * ZC), jnp.bfloat16),
            pltpu.VMEM((32, 256), f32),
            pltpu.VMEM((2, NY * ZC, 32), f32),
            pltpu.VMEM((2, NY * TI, NB * NX, 8, 128), f32),
            pltpu.SMEM((1, 1), jnp.int32),
            pltpu.SMEM((1,), jnp.int32),
            pltpu.VMEM((1, 2 * HALF), f32),
            pltpu.VMEM((NY, NX, TI * TJ, 8, 128), f32),
            pltpu.VMEM((NY * NX, *codes), i16),
            pltpu.VMEM((NY, NX - 1, *codes), i16),
            pltpu.VMEM((OWN - FULL, *codes), i16),
            pltpu.VMEM((OWN, *codes), i16),
            pltpu.VMEM((OWN, *codes), i16),
            pltpu.VMEM((ZC * 8, 128), f32),
            pltpu.VMEM((ZC, 8, 128), i16),
            pltpu.VMEM((ZC, 8, 128), i16),
            pltpu.VMEM((3, 1, 128), f32),
            pltpu.VMEM((NX + NY - 2 + ZC, 1, 128), f32),
            dma((3,)), dma((4,)), pltpu.SemaphoreType.REGULAR((4,)), dma, dma, dma, dma((3,)),
            dma, dma((NY,)), dma, dma((3,)), dma, dma, dma, dma((3,)),
        ],
        compiler_params=pltpu.CompilerParams(collective_id=0, has_side_effects=True),
        name="exchange",
    )(
        partials.reshape(NY, TI, 8, partials.shape[2]),
        scales.reshape(scales.shape[1:]).T,
        overflow_pos,
        exponent.reshape(1),
        weights,
    )
    grad, block_scale, master, new_exponent, count = pl.pallas_call(
        finish,
        out_shape=(
            jax.ShapeDtypeStruct((1, 2 * HALF), f32),
            jax.ShapeDtypeStruct((1, TJ), f32),
            jax.ShapeDtypeStruct((1, 2 * HALF), f32),
            jax.ShapeDtypeStruct((1,), jnp.int32),
            jax.ShapeDtypeStruct((1,), jnp.int32),
        ),
        in_specs=[vmem],
        out_specs=[vmem, vmem, vmem, smem, smem],
        name="finish",
    )(pltpu.with_memory_space_constraint(sums, pltpu.VMEM))
    return grad, block_scale, master, new_exponent.reshape(()), count.reshape(())


def solution(mesh):
    return jax.shard_map(
        on_device,
        mesh=mesh,
        in_specs=(
            P(("inter", "intra"), None, None),
            P(("inter", "intra"), None, None),
            P(("inter", "intra"), None),
            P("inter", "intra"),
            P(),
        ),
        out_specs=(P("inter", "intra"), P("inter", "intra"), P("inter", "intra"), P(), P()),
        check_vma=False,
    )
```

```python
import functools

import jax
import jax.numpy as jnp
from jax import lax
from jax.experimental import pallas as pl
from jax.experimental.pallas import tpu as pltpu
from jax.sharding import PartitionSpec as P

MESH = pl.DeviceIdType.MESH
NX, NY, NZ = 4, 8, 12
ZC = 2 * NZ
TI, TJ = ZC // 8, 5
HALF = TJ * 128
NB = 3
TOP = 32767.0
USED = TI * TJ * 8 + 2
FULL = 3
OWN = NY - 1
SIDES = (1, 3, 2)
SENT = 3 * (FULL + 1) + 2 * (OWN - FULL) + OWN - FULL + OWN


def wait(ref, sem):
    pltpu.make_async_copy(ref, ref, sem).wait()


def far_first(k, n):
    m = (k + 1) // 2
    return jnp.where(k % 2 == 1, n // 2 - m, n // 2 + m)


def top_of(row):
    peak = functools.reduce(jnp.maximum, [jnp.abs(t) for t in row])
    peak = jnp.maximum(jnp.max(peak, axis=1, keepdims=True), 1e-30)
    return jnp.ceil(jnp.log2(jnp.broadcast_to(peak, (8, 128))) + 1e-3)


def code(values):
    return jnp.round(values).astype(jnp.int32).astype(jnp.int16)


def row_lane(i):
    lane = lax.broadcasted_iota(jnp.int32, (8, 128), 1)
    return lane == lax.broadcasted_iota(jnp.int32, (8, 128), 0) + 8 * i


def encode(tiles, tops, out):
    flat, marks = [], jnp.zeros((8, 128), jnp.float32)
    for i in range(TI):
        factor = jnp.exp2(-tops[i]) * TOP
        flat += [t * factor for t in tiles[i]]
        marks = jnp.where(row_lane(i), tops[i], marks)
    flat.append(jnp.broadcast_to(jnp.sum(marks, axis=0, keepdims=True), (8, 128)))
    for p in range(len(flat) // 2):
        out[p * 16 : p * 16 + 16, :] = code(jnp.concatenate([flat[2 * p], flat[2 * p + 1]], axis=0))


def decode(ref):
    flat = []
    for p in range((TI * TJ + 1) // 2):
        pair = ref[p * 16 : p * 16 + 16, :].astype(jnp.int32).astype(jnp.float32)
        flat += [pair[:8], pair[8:]]
    marks = jnp.broadcast_to(flat[TI * TJ][:1], (8, 128))
    tiles = []
    for i in range(TI):
        top = jnp.sum(jnp.where(row_lane(i), marks, 0.0), axis=1, keepdims=True)
        factor = jnp.exp2(jnp.broadcast_to(top, (8, 128))) * (1.0 / TOP)
        tiles.append([flat[i * TJ + j] * factor for j in range(TJ)])
    return tiles


def add(a, b):
    return [[p + q for p, q in zip(r, s)] for r, s in zip(a, b)]


def kernel(
    part, scales, pos, exponent, weights,
    out,
    lev, head, par, sc, st, turned, bx, flag, power, held, terms, cs, xr, dr, ys, yr, zs, zq, zr, fs, fr,
    load_sem, small_sem, near, scale_send, scale_recv, core_send, core_recv,
    part_send, x_recv, early_recv, y_recv, z_send, z_recv, flag_send, flag_recv,
):
    inter, x = lax.axis_index("inter"), lax.axis_index("intra")
    c, zc = inter % 2, inter % ZC
    z, y = zc // 2, inter // ZC
    partner = inter + 1 - 2 * c

    def offset(q):
        return far_first(q, NY)

    def columns(xt, side):
        return pl.ds(pl.multiple_of(xt * 2 * HALF + side * HALF, 128), HALF)

    def load(h, side):
        for xt in range(NX):
            pltpu.make_async_copy(part.at[:, :, :, columns(xt, side)], lev.at[side, :, xt], load_sem.at[h]).start()

    first_y = (y + offset(0)) % NY
    for xt in range(NX):
        pltpu.make_async_copy(part.at[first_y, :, :, columns(xt, c)], head.at[xt], load_sem.at[2]).start()
    pltpu.make_async_copy(scales, sc.at[0], small_sem.at[0]).start()

    barrier = pltpu.get_barrier_semaphore()

    def along_x(d):
        return (inter, (x + d) % NX)

    def along_y(d):
        return ((y + d) % NY * ZC + zc, x)

    def across_y(d):
        return ((y + d) % NY * ZC + zc + 1 - 2 * c, x)

    def along_z(d):
        return (y * ZC + (zc + 2 * d) % ZC, x)

    def tell(sem, to):
        pl.semaphore_signal(sem, inc=1, device_id=to, device_id_type=MESH)

    def tell_both(sem, along, n, d):
        tell(near.at[sem], along(d))
        tell(near.at[sem], along(n - d))

    tell(barrier, (partner, x))
    for d in (1, NX - 1):
        tell(barrier, along_x(d))
    for d in (1, NY - 1):
        tell(barrier, along_y(d))
        tell(barrier, across_y(d))
    for d in (1, NZ - 1):
        tell(barrier, along_z(d))
    load(1, c)
    load(0, 1 - c)
    pltpu.make_async_copy(pos, flag, small_sem.at[1]).start()
    pltpu.make_async_copy(exponent, power, small_sem.at[2]).start()
    pltpu.make_async_copy(weights, held, small_sem.at[3]).start()
    with jax.named_scope("barrier"):
        pl.semaphore_wait(barrier, 1 + 2 + 4 + 2)
    tell_both(3, along_x, NX, 1)
    tell_both(0, along_y, NY, 1)
    tell_both(0, along_z, NZ, 1)

    def core_copy(k, source):
        yt = (y + offset(k)) % NY
        return pltpu.make_async_remote_copy(
            source, par.at[yt], core_send, core_recv.at[(k + 3) // 4], (partner, x), MESH
        )

    scale_copy = pltpu.make_async_remote_copy(
        sc.at[0], sc.at[1], scale_send, scale_recv, (partner, x), MESH
    )
    with jax.named_scope("load"):
        wait(sc.at[0], small_sem.at[0])
        scale_copy.start()
        wait(head, load_sem.at[2])
        core_copy(0, head).start()
        wait(lev.at[c], load_sem.at[1])
        wait(lev.at[1 - c], load_sem.at[0])

    @pl.loop(1, NY)
    def _(k):
        core_copy(k, lev.at[jnp.where(k == OWN, 1 - c, c), (y + offset(k)) % NY]).start()

    def flag_x(d):
        return pltpu.make_async_remote_copy(
            fs.at[0], fr.at[d - 1], flag_send, flag_recv.at[0], along_x(d), MESH
        )

    wait(flag, small_sem.at[1])
    wait(power, small_sem.at[2])
    fs[0] = jnp.full((1, 128), (flag[0, 0] >= 0).astype(jnp.float32), jnp.float32)

    def turn(h):
        st[:20, : NY * ZC] = sc[h].astype(jnp.float32)
        turned[h] = st[...].T[: NY * ZC]

    block = lax.broadcasted_iota(jnp.int32, (32, 128), 0)

    def spread(h, first, n, side):
        rows = turned[h, pl.ds(pl.multiple_of(first * 8, 8), n * 8), :].astype(jnp.bfloat16)
        for t in range(0, NB * NX, 2):
            picks = [
                jnp.where(block == u // NB * TJ + 2 * side + u % NB, 1.0, 0.0).astype(jnp.bfloat16)
                for u in (t, t + 1)
            ]
            both = jnp.dot(rows, jnp.concatenate(picks, axis=1), preferred_element_type=jnp.float32)
            for u in range(2):
                bx[h, pl.ds(first, n), t + u] = both[:, u * 128 : (u + 1) * 128].reshape(n, 8, 128)

    st[...] = jnp.zeros((32, 256), jnp.float32)
    with jax.named_scope("spread0"):
        turn(0)
        spread(0, 0, NY * TI, 1 - c)
        spread(0, y * TI, TI, c)
    with jax.named_scope("wait_scale"):
        scale_copy.wait()
    with jax.named_scope("turn"):
        turn(1)

    def x_copy(src, k, d):
        return pltpu.make_async_remote_copy(
            src.at[:USED], xr.at[k, SIDES.index(d), :USED], part_send, x_recv.at[k], along_x(d), MESH
        )

    def early_copy(q):
        return pltpu.make_async_remote_copy(
            cs.at[q * NX + 2, :USED], dr.at[q - FULL, :USED], part_send, early_recv, across_y(offset(q)), MESH
        )

    def tiles_of(q, d):
        return [[terms[q, d, i * TJ + j] for j in range(TJ)] for i in range(TI)]

    with jax.named_scope("near_x"):
        pl.semaphore_wait(near.at[3], 2)
    for d in range(1, NX):
        flag_x(d).start()
    with jax.named_scope("spread1"):
        spread(1, (y + offset(0)) % NY * TI, TI, 1 - c)

    def produce(q):
        yt = (y + offset(q)) % NY
        for g, (first, n) in enumerate(((0, 1), (1, 4), (5, 3))):

            @pl.when(q == first)
            def _():
                with jax.named_scope("wait_core"):
                    wait(par.at[:n], core_recv.at[g])

        side = jnp.where(q == OWN, c, 1 - c)
        even = side == 0
        tops = []
        for d in range(NX):
            xt = (x + d) % NX
            for i in range(TI):
                row = None
                for h in range(2):
                    b = [bx[h, yt * TI + i, xt * NB + n] for n in range(NB)]
                    b = [b[0], jnp.where(even, b[0], b[1]), b[1], jnp.where(even, b[1], b[2]), b[2]]
                    levels = par[yt, xt, i] if h else lev[side, yt, xt, i]
                    levels = levels.astype(jnp.float32)
                    term = [levels[:, j * 128 : (j + 1) * 128] * b[j] for j in range(TJ)]
                    row = term if row is None else [p + q for p, q in zip(row, term)]
                for j in range(TJ):
                    terms[q, d, i * TJ + j] = row[j]
                tops.append(top_of(row))

        def send(d):
            encode(tiles_of(q, d), tops[d * TI : d * TI + TI], cs.at[q * NX + d])

        @pl.when(q < FULL)
        def _():
            send(2)
            x_copy(cs.at[q * NX + 2], q, 2).start()

        @pl.when(jnp.logical_and(q >= FULL, q < OWN))
        def _():
            send(2)
            early_copy(q).start()

        for d in (1, 3):
            send(d)
            x_copy(cs.at[q * NX + d], q, d).start()

        @pl.when(q == FULL - 1)
        def _():
            with jax.named_scope("near0"):
                pl.semaphore_wait(near.at[0], 4)
            tell_both(1, along_y, NY, 2)
            tell_both(1, along_z, NZ, 2)

    @pl.loop(0, NY)
    def _(q):
        produce(q)

        @pl.when(q == 0)
        def _():
            spread(1, 0, NY * TI, 1 - c)
            spread(1, y * TI, TI, c)

    flags = fs[0]
    wait(fr.at[: NX - 1], flag_recv.at[0])
    for n in range(NX - 1):
        flags = flags + fr[n]
    fs[1] = flags
    with jax.named_scope("near"):
        pl.semaphore_wait(near.at[1], 4)
    tell_both(2, along_z, NZ, 4)

    def flag_y(d):
        return pltpu.make_async_remote_copy(
            fs.at[1], fr.at[NX + d - 2], flag_send, flag_recv.at[1], across_y(d), MESH
        )

    for d in range(1, NY):
        flag_y(d).start()

    def y_copy(k):
        return pltpu.make_async_remote_copy(
            ys.at[k, :USED], yr.at[k, :USED], part_send, y_recv.at[jnp.maximum(k - 4, 0)], across_y(offset(k)), MESH
        )

    def x_sum(k, n):
        with jax.named_scope("wait_x"):
            wait(xr.at[k, :n, :USED], x_recv.at[k])
        tiles = tiles_of(k, 0)
        for m in range(n):
            tiles = add(tiles, decode(xr.at[k, m]))
        return tiles

    def flag_z(k):
        to = (zc + far_first(k, ZC)) % ZC
        return pltpu.make_async_remote_copy(
            fs.at[2], fr.at[NX + NY - 2 + zc], flag_send, flag_recv.at[2], (y * ZC + to, x), MESH
        )

    def pass_on(k, n):
        tiles = x_sum(k, n)
        encode(tiles, [top_of(row) for row in tiles], ys.at[k])
        y_copy(k).start()

    @pl.loop(0, FULL - 1)
    def _(k):
        pass_on(k, 3)

    tiles = tiles_of(OWN, 2)
    with jax.named_scope("wait_d"):
        wait(dr.at[:, :USED], early_recv)
    for n in range(OWN - FULL):
        tiles = add(tiles, decode(dr.at[n]))
    encode(tiles, [top_of(row) for row in tiles], cs.at[OWN * NX + 2])
    x_copy(cs.at[OWN * NX + 2], OWN, 2).start()

    pass_on(FULL - 1, 3)

    @pl.loop(FULL, OWN)
    def _(k):
        pass_on(k, 2)

    flags = fs[1]
    with jax.named_scope("wait_fy"):
        wait(fr.at[NX - 1 : NX + NY - 2], flag_recv.at[1])
    for n in range(NX - 1, NX + NY - 2):
        flags = flags + fr[n]
    fs[2] = flags
    fr[NX + NY - 2 + zc] = flags
    with jax.named_scope("near4"):
        pl.semaphore_wait(near.at[2], 2)

    @pl.loop(0, ZC - 1)
    def _(n):
        flag_z(n).start()

    tiles = x_sum(OWN, 3)
    for g, (first, n) in enumerate(((0, 5), (5, 1), (6, 1))):
        with jax.named_scope("wait_y"):
            wait(yr.at[first : first + n, :USED], y_recv.at[g])
        for k in range(first, first + n):
            tiles = add(tiles, decode(yr.at[k]))
    for i in range(TI):
        top = top_of(tiles[i])
        factor = jnp.exp2(-top) * TOP
        for j in range(TJ):
            zs[pl.ds(i * 64 + j, 8, stride=8), :] = tiles[i][j] * factor
        zs[pl.ds(i * 64 + TJ, 8, stride=8), :] = top
    for r in range(ZC):
        zq[r] = code(zs[r * 8 : r * 8 + 8, :])

    def z_copy(k):
        to = (zc + far_first(k, ZC)) % ZC
        return pltpu.make_async_remote_copy(
            zq.at[to, : TJ + 1], zr.at[zc, : TJ + 1], z_send, z_recv, (y * ZC + to, x), MESH
        )

    @pl.loop(0, ZC - 1)
    def _(k):
        z_copy(k).start()

    zr[zc] = zq[zc]

    wait(held, small_sem.at[3])
    for h in range(2):
        for j in range(TJ):
            at = (h * TJ + j) * 128
            out[16 + h * 8 + j : 17 + h * 8 + j, :] = held[:, at : at + 128]

    wait(lev.at[1], core_send)
    wait(cs.at[:SENT, :USED], part_send)
    wait(fr.at[: NX + NY + ZC - 3], flag_send)
    with jax.named_scope("wait_flags"):
        wait(fr.at[NX + NY - 2 : NX + NY + ZC - 3], flag_recv.at[2])
    count = functools.reduce(jnp.add, [fr[NX + NY - 2 + n] for n in range(ZC)])
    with jax.named_scope("wait_z"):
        wait(zr.at[: ZC - 1, : TJ + 1], z_recv)

    def row_sum(n, totals):
        sums = []
        for h in range(2):
            codes = zr[2 * n + h].astype(jnp.int32).astype(jnp.float32)
            factor = jnp.exp2(jnp.broadcast_to(codes[TJ : TJ + 1], (8, 128))) * (1.0 / TOP)
            sums.append(totals[h] + codes * factor)
        return tuple(sums)

    zero = jnp.zeros((8, 128), jnp.float32)
    totals = lax.fori_loop(0, NZ, row_sum, (zero, zero), unroll=4)
    for h in range(2):
        out[h * 8 : h * 8 + TJ, :] = totals[h][:TJ]
    out[TJ : TJ + 1, :] = count
    out[7:8, :] = jnp.full((1, 128), power[0].astype(jnp.float32), jnp.float32)
    wait(zr.at[: ZC - 1, : TJ + 1], z_send)


def finish(sums, grad, block_scale, master, new_exponent, count):
    flagged = sums[TJ, 0].astype(jnp.int32)
    factor = jnp.exp2(-jnp.broadcast_to(sums[7:8, :], (8, 128)))
    peaks = []
    for h in range(2):
        g = sums[h * 8 : h * 8 + 8, :] * factor
        peak = jnp.max(jnp.abs(g), axis=1, keepdims=True)
        for j in range(TJ):
            at = slice((h * TJ + j) * 128, (h * TJ + j + 1) * 128)
            w = sums[16 + h * 8 + j : 17 + h * 8 + j, :]
            grad[:, at] = g[j : j + 1]
            master[:, at] = jnp.where(flagged == 0, w - 0.5 * g[j : j + 1], w)
            peaks.append(peak[j : j + 1])
    lane = lax.broadcasted_iota(jnp.int32, (1, 128), 1)
    scale = jnp.zeros((1, 128), jnp.float32)
    for b in range(TJ):
        top = jnp.maximum(peaks[2 * b], peaks[2 * b + 1]) / 127.0
        scale = jnp.where(lane == b, jnp.broadcast_to(top, (1, 128)), scale)
    block_scale[...] = scale[:, :TJ]
    new_exponent[0] = sums[7, 0].astype(jnp.int32) - (flagged > 0).astype(jnp.int32)
    count[0] = flagged


def on_device(partials, scales, overflow_pos, weights, exponent):
    vmem, smem, hbm = (
        pl.BlockSpec(memory_space=m) for m in (pltpu.VMEM, pltpu.SMEM, pltpu.HBM)
    )
    f32, i16, dma = jnp.float32, jnp.int16, pltpu.SemaphoreType.DMA
    codes = (128, 128)
    sums = pl.pallas_call(
        kernel,
        out_shape=pltpu.VMEM((32, 128), f32),
        in_specs=[hbm] * 5,
        out_specs=vmem,
        scratch_shapes=[
            pltpu.VMEM((2, NY, NX, TI, 8, HALF), jnp.bfloat16),
            pltpu.VMEM((NX, TI, 8, HALF), jnp.bfloat16),
            pltpu.VMEM((NY, NX, TI, 8, HALF), jnp.bfloat16),
            pltpu.VMEM((2, 20, NY * ZC), jnp.bfloat16),
            pltpu.VMEM((32, 256), f32),
            pltpu.VMEM((2, NY * ZC, 32), f32),
            pltpu.VMEM((2, NY * TI, NB * NX, 8, 128), f32),
            pltpu.SMEM((1, 1), jnp.int32),
            pltpu.SMEM((1,), jnp.int32),
            pltpu.VMEM((1, 2 * HALF), f32),
            pltpu.VMEM((NY, NX, TI * TJ, 8, 128), f32),
            pltpu.VMEM((NY * NX, *codes), i16),
            pltpu.VMEM((NY, NX - 1, *codes), i16),
            pltpu.VMEM((OWN - FULL, *codes), i16),
            pltpu.VMEM((OWN, *codes), i16),
            pltpu.VMEM((OWN, *codes), i16),
            pltpu.VMEM((ZC * 8, 128), f32),
            pltpu.VMEM((ZC, 8, 128), i16),
            pltpu.VMEM((ZC, 8, 128), i16),
            pltpu.VMEM((3, 1, 128), f32),
            pltpu.VMEM((NX + NY - 2 + ZC, 1, 128), f32),
            dma((3,)), dma((4,)), pltpu.SemaphoreType.REGULAR((4,)), dma, dma, dma, dma((3,)),
            dma, dma((NY,)), dma, dma((3,)), dma, dma, dma, dma((3,)),
        ],
        compiler_params=pltpu.CompilerParams(collective_id=0, has_side_effects=True),
        name="exchange",
    )(
        partials.reshape(NY, TI, 8, partials.shape[2]),
        scales.reshape(scales.shape[1:]).T,
        overflow_pos,
        exponent.reshape(1),
        weights,
    )
    grad, block_scale, master, new_exponent, count = pl.pallas_call(
        finish,
        out_shape=(
            jax.ShapeDtypeStruct((1, 2 * HALF), f32),
            jax.ShapeDtypeStruct((1, TJ), f32),
            jax.ShapeDtypeStruct((1, 2 * HALF), f32),
            jax.ShapeDtypeStruct((1,), jnp.int32),
            jax.ShapeDtypeStruct((1,), jnp.int32),
        ),
        in_specs=[vmem],
        out_specs=[vmem, vmem, vmem, smem, smem],
        name="finish",
    )(pltpu.with_memory_space_constraint(sums, pltpu.VMEM))
    return grad, block_scale, master, new_exponent.reshape(()), count.reshape(())


def solution(mesh):
    return jax.shard_map(
        on_device,
        mesh=mesh,
        in_specs=(
            P(("inter", "intra"), None, None),
            P(("inter", "intra"), None, None),
            P(("inter", "intra"), None),
            P("inter", "intra"),
            P(),
        ),
        out_specs=(P("inter", "intra"), P("inter", "intra"), P("inter", "intra"), P(), P()),
        check_vma=False,
    )
```

```python
import functools

import jax
import jax.numpy as jnp
from jax import lax
from jax.experimental import pallas as pl
from jax.experimental.pallas import tpu as pltpu
from jax.sharding import PartitionSpec as P

MESH = pl.DeviceIdType.MESH
NX, NY, NZ = 4, 8, 12
ZC = 2 * NZ
TI, TJ = ZC // 8, 5
HALF = TJ * 128
NB = 3
TOP = 32767.0
USED = TI * TJ * 8 + 2
FULL = 3
OWN = NY - 1
SIDES = (1, 3, 2)
SENT = 3 * (FULL + 1) + 2 * (OWN - FULL) + OWN - FULL + OWN


def wait(ref, sem):
    pltpu.make_async_copy(ref, ref, sem).wait()


def far_first(k, n):
    m = (k + 1) // 2
    return jnp.where(k % 2 == 1, n // 2 - m, n // 2 + m)


def top_of(row):
    peak = functools.reduce(jnp.maximum, [jnp.abs(t) for t in row])
    peak = jnp.maximum(jnp.max(peak, axis=1, keepdims=True), 1e-30)
    return jnp.ceil(jnp.log2(jnp.broadcast_to(peak, (8, 128))) + 1e-3)


def code(values):
    return jnp.round(values).astype(jnp.int32).astype(jnp.int16)


def row_lane(i):
    lane = lax.broadcasted_iota(jnp.int32, (8, 128), 1)
    return lane == lax.broadcasted_iota(jnp.int32, (8, 128), 0) + 8 * i


def encode(tiles, tops, out):
    flat, marks = [], jnp.zeros((8, 128), jnp.float32)
    for i in range(TI):
        factor = jnp.exp2(-tops[i]) * TOP
        flat += [t * factor for t in tiles[i]]
        marks = jnp.where(row_lane(i), tops[i], marks)
    flat.append(jnp.broadcast_to(jnp.sum(marks, axis=0, keepdims=True), (8, 128)))
    for p in range(len(flat) // 2):
        out[p * 16 : p * 16 + 16, :] = code(jnp.concatenate([flat[2 * p], flat[2 * p + 1]], axis=0))


def decode(ref):
    flat = []
    for p in range((TI * TJ + 1) // 2):
        pair = ref[p * 16 : p * 16 + 16, :].astype(jnp.int32).astype(jnp.float32)
        flat += [pair[:8], pair[8:]]
    marks = jnp.broadcast_to(flat[TI * TJ][:1], (8, 128))
    tiles = []
    for i in range(TI):
        top = jnp.sum(jnp.where(row_lane(i), marks, 0.0), axis=1, keepdims=True)
        factor = jnp.exp2(jnp.broadcast_to(top, (8, 128))) * (1.0 / TOP)
        tiles.append([flat[i * TJ + j] * factor for j in range(TJ)])
    return tiles


def add(a, b):
    return [[p + q for p, q in zip(r, s)] for r, s in zip(a, b)]


def kernel(
    part, scales, pos, exponent, weights,
    out,
    lev, head, par, sc, st, turned, bx, flag, power, held, terms, cs, xr, dr, ys, yr, zs, zq, zr, fs, fr,
    load_sem, small_sem, near, scale_send, scale_recv, core_send, core_recv,
    part_send, x_recv, early_recv, y_recv, z_send, z_recv, flag_send, flag_recv,
):
    inter, x = lax.axis_index("inter"), lax.axis_index("intra")
    c, zc = inter % 2, inter % ZC
    z, y = zc // 2, inter // ZC
    partner = inter + 1 - 2 * c

    def offset(q):
        return far_first(q, NY)

    def columns(xt, side):
        return pl.ds(pl.multiple_of(xt * 2 * HALF + side * HALF, 128), HALF)

    def load(h, side):
        for xt in range(NX):
            pltpu.make_async_copy(part.at[:, :, :, columns(xt, side)], lev.at[side, :, xt], load_sem.at[h]).start()

    first_y = (y + offset(0)) % NY
    for xt in range(NX):
        pltpu.make_async_copy(part.at[first_y, :, :, columns(xt, c)], head.at[xt], load_sem.at[2]).start()
    pltpu.make_async_copy(scales, sc.at[0], small_sem.at[0]).start()

    barrier = pltpu.get_barrier_semaphore()

    def along_x(d):
        return (inter, (x + d) % NX)

    def along_y(d):
        return ((y + d) % NY * ZC + zc, x)

    def across_y(d):
        return ((y + d) % NY * ZC + zc + 1 - 2 * c, x)

    def along_z(d):
        return (y * ZC + (zc + 2 * d) % ZC, x)

    def tell(sem, to):
        pl.semaphore_signal(sem, inc=1, device_id=to, device_id_type=MESH)

    def tell_both(sem, along, n, d):
        tell(near.at[sem], along(d))
        tell(near.at[sem], along(n - d))

    tell(barrier, (partner, x))
    for d in (1, NX - 1):
        tell(barrier, along_x(d))
    for d in (1, NY - 1):
        tell(barrier, along_y(d))
        tell(barrier, across_y(d))
    for d in (1, NZ - 1):
        tell(barrier, along_z(d))
    load(1, c)
    load(0, 1 - c)
    pltpu.make_async_copy(pos, flag, small_sem.at[1]).start()
    pltpu.make_async_copy(exponent, power, small_sem.at[2]).start()
    pltpu.make_async_copy(weights, held, small_sem.at[3]).start()
    with jax.named_scope("barrier"):
        pl.semaphore_wait(barrier, 1 + 2 + 4 + 2)
    tell_both(3, along_x, NX, 1)
    tell_both(0, along_y, NY, 1)
    tell_both(0, along_z, NZ, 1)

    def core_copy(k, source):
        yt = (y + offset(k)) % NY
        return pltpu.make_async_remote_copy(
            source, par.at[yt], core_send, core_recv.at[(k + 3) // 4], (partner, x), MESH
        )

    scale_copy = pltpu.make_async_remote_copy(
        sc.at[0], sc.at[1], scale_send, scale_recv, (partner, x), MESH
    )
    with jax.named_scope("load"):
        wait(sc.at[0], small_sem.at[0])
        scale_copy.start()
        wait(head, load_sem.at[2])
        core_copy(0, head).start()
        wait(lev.at[c], load_sem.at[1])
        wait(lev.at[1 - c], load_sem.at[0])

    @pl.loop(1, NY)
    def _(k):
        core_copy(k, lev.at[jnp.where(k == OWN, 1 - c, c), (y + offset(k)) % NY]).start()

    def flag_x(d):
        return pltpu.make_async_remote_copy(
            fs.at[0], fr.at[d - 1], flag_send, flag_recv.at[0], along_x(d), MESH
        )

    wait(flag, small_sem.at[1])
    wait(power, small_sem.at[2])
    fs[0] = jnp.full((1, 128), (flag[0, 0] >= 0).astype(jnp.float32), jnp.float32)

    def turn(h):
        st[:20, : NY * ZC] = sc[h].astype(jnp.float32)
        turned[h] = st[...].T[: NY * ZC]

    block = lax.broadcasted_iota(jnp.int32, (32, 128), 0)

    def spread(h, first, n, side):
        rows = turned[h, pl.ds(pl.multiple_of(first * 8, 8), n * 8), :].astype(jnp.bfloat16)
        for t in range(0, NB * NX, 2):
            picks = [
                jnp.where(block == u // NB * TJ + 2 * side + u % NB, 1.0, 0.0).astype(jnp.bfloat16)
                for u in (t, t + 1)
            ]
            both = jnp.dot(rows, jnp.concatenate(picks, axis=1), preferred_element_type=jnp.float32)
            for u in range(2):
                bx[h, pl.ds(first, n), t + u] = both[:, u * 128 : (u + 1) * 128].reshape(n, 8, 128)

    st[...] = jnp.zeros((32, 256), jnp.float32)
    with jax.named_scope("spread0"):
        turn(0)
        spread(0, 0, NY * TI, 1 - c)
        spread(0, y * TI, TI, c)
    with jax.named_scope("wait_scale"):
        scale_copy.wait()
    with jax.named_scope("turn"):
        turn(1)

    def x_copy(src, k, d):
        return pltpu.make_async_remote_copy(
            src.at[:USED], xr.at[k, SIDES.index(d), :USED], part_send, x_recv.at[k], along_x(d), MESH
        )

    def early_copy(q):
        return pltpu.make_async_remote_copy(
            cs.at[q * NX + 2, :USED], dr.at[q - FULL, :USED], part_send, early_recv, across_y(offset(q)), MESH
        )

    def tiles_of(q, d):
        return [[terms[q, d, i * TJ + j] for j in range(TJ)] for i in range(TI)]

    with jax.named_scope("spread1"):
        spread(1, (y + offset(0)) % NY * TI, TI, 1 - c)

    def produce(q):
        yt = (y + offset(q)) % NY
        for g, (first, n) in enumerate(((0, 1), (1, 4), (5, 3))):

            @pl.when(q == first)
            def _():
                with jax.named_scope("wait_core"):
                    wait(par.at[:n], core_recv.at[g])

        side = jnp.where(q == OWN, c, 1 - c)
        even = side == 0
        tops = []
        for d in range(NX):
            xt = (x + d) % NX
            for i in range(TI):
                row = None
                for h in range(2):
                    b = [bx[h, yt * TI + i, xt * NB + n] for n in range(NB)]
                    b = [b[0], jnp.where(even, b[0], b[1]), b[1], jnp.where(even, b[1], b[2]), b[2]]
                    levels = par[yt, xt, i] if h else lev[side, yt, xt, i]
                    levels = levels.astype(jnp.float32)
                    term = [levels[:, j * 128 : (j + 1) * 128] * b[j] for j in range(TJ)]
                    row = term if row is None else [p + q for p, q in zip(row, term)]
                for j in range(TJ):
                    terms[q, d, i * TJ + j] = row[j]
                tops.append(top_of(row))

        def send(d):
            encode(tiles_of(q, d), tops[d * TI : d * TI + TI], cs.at[q * NX + d])

        @pl.when(q < FULL)
        def _():
            send(2)

            @pl.when(q == 0)
            def _():
                with jax.named_scope("near_x"):
                    pl.semaphore_wait(near.at[3], 2)
                for d in range(1, NX):
                    flag_x(d).start()

            x_copy(cs.at[q * NX + 2], q, 2).start()

        @pl.when(jnp.logical_and(q >= FULL, q < OWN))
        def _():
            send(2)
            early_copy(q).start()

        for d in (1, 3):
            send(d)
            x_copy(cs.at[q * NX + d], q, d).start()

        @pl.when(q == FULL - 1)
        def _():
            with jax.named_scope("near0"):
                pl.semaphore_wait(near.at[0], 4)
            tell_both(1, along_y, NY, 2)
            tell_both(1, along_z, NZ, 2)

    @pl.loop(0, NY)
    def _(q):
        produce(q)

        @pl.when(q == 0)
        def _():
            spread(1, 0, NY * TI, 1 - c)
            spread(1, y * TI, TI, c)

    flags = fs[0]
    wait(fr.at[: NX - 1], flag_recv.at[0])
    for n in range(NX - 1):
        flags = flags + fr[n]
    fs[1] = flags
    with jax.named_scope("near"):
        pl.semaphore_wait(near.at[1], 4)
    tell_both(2, along_z, NZ, 4)

    def flag_y(d):
        return pltpu.make_async_remote_copy(
            fs.at[1], fr.at[NX + d - 2], flag_send, flag_recv.at[1], across_y(d), MESH
        )

    for d in range(1, NY):
        flag_y(d).start()

    def y_copy(k):
        return pltpu.make_async_remote_copy(
            ys.at[k, :USED], yr.at[k, :USED], part_send, y_recv.at[jnp.maximum(k - 4, 0)], across_y(offset(k)), MESH
        )

    def x_sum(k, n):
        with jax.named_scope("wait_x"):
            wait(xr.at[k, :n, :USED], x_recv.at[k])
        tiles = tiles_of(k, 0)
        for m in range(n):
            tiles = add(tiles, decode(xr.at[k, m]))
        return tiles

    def flag_z(k):
        to = (zc + far_first(k, ZC)) % ZC
        return pltpu.make_async_remote_copy(
            fs.at[2], fr.at[NX + NY - 2 + zc], flag_send, flag_recv.at[2], (y * ZC + to, x), MESH
        )

    def pass_on(k, n):
        tiles = x_sum(k, n)
        encode(tiles, [top_of(row) for row in tiles], ys.at[k])
        y_copy(k).start()

    @pl.loop(0, FULL - 1)
    def _(k):
        pass_on(k, 3)

    tiles = tiles_of(OWN, 2)
    with jax.named_scope("wait_d"):
        wait(dr.at[:, :USED], early_recv)
    for n in range(OWN - FULL):
        tiles = add(tiles, decode(dr.at[n]))
    encode(tiles, [top_of(row) for row in tiles], cs.at[OWN * NX + 2])
    x_copy(cs.at[OWN * NX + 2], OWN, 2).start()

    pass_on(FULL - 1, 3)

    @pl.loop(FULL, OWN)
    def _(k):
        pass_on(k, 2)

    flags = fs[1]
    with jax.named_scope("wait_fy"):
        wait(fr.at[NX - 1 : NX + NY - 2], flag_recv.at[1])
    for n in range(NX - 1, NX + NY - 2):
        flags = flags + fr[n]
    fs[2] = flags
    fr[NX + NY - 2 + zc] = flags
    with jax.named_scope("near4"):
        pl.semaphore_wait(near.at[2], 2)

    @pl.loop(0, ZC - 1)
    def _(n):
        flag_z(n).start()

    tiles = x_sum(OWN, 3)
    for g, (first, n) in enumerate(((0, 5), (5, 1), (6, 1))):
        with jax.named_scope("wait_y"):
            wait(yr.at[first : first + n, :USED], y_recv.at[g])
        for k in range(first, first + n):
            tiles = add(tiles, decode(yr.at[k]))
    for i in range(TI):
        top = top_of(tiles[i])
        factor = jnp.exp2(-top) * TOP
        for j in range(TJ):
            zs[pl.ds(i * 64 + j, 8, stride=8), :] = tiles[i][j] * factor
        zs[pl.ds(i * 64 + TJ, 8, stride=8), :] = top
    for r in range(ZC):
        zq[r] = code(zs[r * 8 : r * 8 + 8, :])

    def z_copy(k):
        to = (zc + far_first(k, ZC)) % ZC
        return pltpu.make_async_remote_copy(
            zq.at[to, : TJ + 1], zr.at[zc, : TJ + 1], z_send, z_recv, (y * ZC + to, x), MESH
        )

    @pl.loop(0, ZC - 1)
    def _(k):
        z_copy(k).start()

    zr[zc] = zq[zc]

    wait(held, small_sem.at[3])
    for h in range(2):
        for j in range(TJ):
            at = (h * TJ + j) * 128
            out[16 + h * 8 + j : 17 + h * 8 + j, :] = held[:, at : at + 128]

    wait(lev.at[1], core_send)
    wait(cs.at[:SENT, :USED], part_send)
    wait(fr.at[: NX + NY + ZC - 3], flag_send)
    with jax.named_scope("wait_flags"):
        wait(fr.at[NX + NY - 2 : NX + NY + ZC - 3], flag_recv.at[2])
    count = functools.reduce(jnp.add, [fr[NX + NY - 2 + n] for n in range(ZC)])
    with jax.named_scope("wait_z"):
        wait(zr.at[: ZC - 1, : TJ + 1], z_recv)

    def row_sum(n, totals):
        sums = []
        for h in range(2):
            codes = zr[2 * n + h].astype(jnp.int32).astype(jnp.float32)
            factor = jnp.exp2(jnp.broadcast_to(codes[TJ : TJ + 1], (8, 128))) * (1.0 / TOP)
            sums.append(totals[h] + codes * factor)
        return tuple(sums)

    zero = jnp.zeros((8, 128), jnp.float32)
    totals = lax.fori_loop(0, NZ, row_sum, (zero, zero), unroll=4)
    for h in range(2):
        out[h * 8 : h * 8 + TJ, :] = totals[h][:TJ]
    out[TJ : TJ + 1, :] = count
    out[7:8, :] = jnp.full((1, 128), power[0].astype(jnp.float32), jnp.float32)
    wait(zr.at[: ZC - 1, : TJ + 1], z_send)


def finish(sums, grad, block_scale, master, new_exponent, count):
    flagged = sums[TJ, 0].astype(jnp.int32)
    factor = jnp.exp2(-jnp.broadcast_to(sums[7:8, :], (8, 128)))
    peaks = []
    for h in range(2):
        g = sums[h * 8 : h * 8 + 8, :] * factor
        peak = jnp.max(jnp.abs(g), axis=1, keepdims=True)
        for j in range(TJ):
            at = slice((h * TJ + j) * 128, (h * TJ + j + 1) * 128)
            w = sums[16 + h * 8 + j : 17 + h * 8 + j, :]
            grad[:, at] = g[j : j + 1]
            master[:, at] = jnp.where(flagged == 0, w - 0.5 * g[j : j + 1], w)
            peaks.append(peak[j : j + 1])
    lane = lax.broadcasted_iota(jnp.int32, (1, 128), 1)
    scale = jnp.zeros((1, 128), jnp.float32)
    for b in range(TJ):
        top = jnp.maximum(peaks[2 * b], peaks[2 * b + 1]) / 127.0
        scale = jnp.where(lane == b, jnp.broadcast_to(top, (1, 128)), scale)
    block_scale[...] = scale[:, :TJ]
    new_exponent[0] = sums[7, 0].astype(jnp.int32) - (flagged > 0).astype(jnp.int32)
    count[0] = flagged


def on_device(partials, scales, overflow_pos, weights, exponent):
    vmem, smem, hbm = (
        pl.BlockSpec(memory_space=m) for m in (pltpu.VMEM, pltpu.SMEM, pltpu.HBM)
    )
    f32, i16, dma = jnp.float32, jnp.int16, pltpu.SemaphoreType.DMA
    codes = (128, 128)
    sums = pl.pallas_call(
        kernel,
        out_shape=pltpu.VMEM((32, 128), f32),
        in_specs=[hbm] * 5,
        out_specs=vmem,
        scratch_shapes=[
            pltpu.VMEM((2, NY, NX, TI, 8, HALF), jnp.bfloat16),
            pltpu.VMEM((NX, TI, 8, HALF), jnp.bfloat16),
            pltpu.VMEM((NY, NX, TI, 8, HALF), jnp.bfloat16),
            pltpu.VMEM((2, 20, NY * ZC), jnp.bfloat16),
            pltpu.VMEM((32, 256), f32),
            pltpu.VMEM((2, NY * ZC, 32), f32),
            pltpu.VMEM((2, NY * TI, NB * NX, 8, 128), f32),
            pltpu.SMEM((1, 1), jnp.int32),
            pltpu.SMEM((1,), jnp.int32),
            pltpu.VMEM((1, 2 * HALF), f32),
            pltpu.VMEM((NY, NX, TI * TJ, 8, 128), f32),
            pltpu.VMEM((NY * NX, *codes), i16),
            pltpu.VMEM((NY, NX - 1, *codes), i16),
            pltpu.VMEM((OWN - FULL, *codes), i16),
            pltpu.VMEM((OWN, *codes), i16),
            pltpu.VMEM((OWN, *codes), i16),
            pltpu.VMEM((ZC * 8, 128), f32),
            pltpu.VMEM((ZC, 8, 128), i16),
            pltpu.VMEM((ZC, 8, 128), i16),
            pltpu.VMEM((3, 1, 128), f32),
            pltpu.VMEM((NX + NY - 2 + ZC, 1, 128), f32),
            dma((3,)), dma((4,)), pltpu.SemaphoreType.REGULAR((4,)), dma, dma, dma, dma((3,)),
            dma, dma((NY,)), dma, dma((3,)), dma, dma, dma, dma((3,)),
        ],
        compiler_params=pltpu.CompilerParams(collective_id=0, has_side_effects=True),
        name="exchange",
    )(
        partials.reshape(NY, TI, 8, partials.shape[2]),
        scales.reshape(scales.shape[1:]).T,
        overflow_pos,
        exponent.reshape(1),
        weights,
    )
    grad, block_scale, master, new_exponent, count = pl.pallas_call(
        finish,
        out_shape=(
            jax.ShapeDtypeStruct((1, 2 * HALF), f32),
            jax.ShapeDtypeStruct((1, TJ), f32),
            jax.ShapeDtypeStruct((1, 2 * HALF), f32),
            jax.ShapeDtypeStruct((1,), jnp.int32),
            jax.ShapeDtypeStruct((1,), jnp.int32),
        ),
        in_specs=[vmem],
        out_specs=[vmem, vmem, vmem, smem, smem],
        name="finish",
    )(pltpu.with_memory_space_constraint(sums, pltpu.VMEM))
    return grad, block_scale, master, new_exponent.reshape(()), count.reshape(())


def solution(mesh):
    return jax.shard_map(
        on_device,
        mesh=mesh,
        in_specs=(
            P(("inter", "intra"), None, None),
            P(("inter", "intra"), None, None),
            P(("inter", "intra"), None),
            P("inter", "intra"),
            P(),
        ),
        out_specs=(P("inter", "intra"), P("inter", "intra"), P("inter", "intra"), P(), P()),
        check_vma=False,
    )
```
